128 devices in a mesh: ctx: 32 (over x, y, core), head: 4 (over z).
Axes of the slice: x: 4, y: 4, z: 4, core: 2. Of those that a mesh axis runs over, the one named last changes fastest.
Arguments:
- query: bfloat16 [32768, 4096], P('ctx', 'head'), may hold values from -150 to 150
- keys: bfloat16 [32768, 4096], P('ctx', 'head'), may hold values from -5.5 to 5.5, as said below
- values: bfloat16 [32768, 4096], P('ctx', 'head'), may hold values from -6 to 6
- lr_code: int32 [32768, 8], P('ctx', 'head'), may hold values from 2048 to 26623, as said below
- fast_weights: bfloat16 [8, 3, 512, 512], P('head'), may hold values from -0.25 to 0.25
- out_weight: bfloat16 [4096, 4096], P('head'), may hold values from -0.09375 to 0.09375
Outputs:
- layer_out: bfloat16 [32768, 4096], P('ctx', 'head')
- new_weights: bfloat16 [8, 3, 512, 512], P('head')
The draws below stay inside these ranges and needn't reach their ends.
Inputs may be any that keep to these rules, and one draw needn't show every extreme that they name: `keys`: keys of order one. `lr_code`: Fixed-point learning-rate codes in units of 2**-14.
All inputs are finite; a program needn't handle non-finite values.
Results may differ from the reference program's by a relative error of at most 0.025.
Values may be sent and summed in bfloat16 or wider, within the bound.
A program may use at most 192 MiB of HBM per device.

```python
import math
import jax
import jax.numpy as jnp
from jax import lax

D = 4096
FW = 512
FHEADS = 8
HEAD_DIM = 128
WINDOW = 256
TOKENS = 32768
N_HEAD = 4


def pair_draw(key):
    key_k = jax.random.fold_in(key, 101)
    key_q = jax.random.fold_in(key, 202)
    keys_drawn = jnp.clip(jax.random.normal(key_k, (TOKENS, D), jnp.float32), -5.0, 5.0)
    query_drawn = jnp.clip(jax.random.normal(key_q, (TOKENS, D), jnp.float32), -5.0, 5.0)
    return (query_drawn, keys_drawn)


def draw_query(key, part):
    return pair_draw(key)[0].astype(jnp.bfloat16)


def draw_keys(key, part):
    return pair_draw(key)[1].astype(jnp.bfloat16)


def draw_lr_code(key, part):
    position = jnp.arange(TOKENS, dtype=jnp.int32)[:, None]
    spread = jax.random.randint(jax.random.fold_in(key, 505), (TOKENS, FHEADS), 0, 8192, jnp.int32)
    return 2048 + spread + position * 16384 // TOKENS


def shard_levels(rng, shape, cuts, smallest, high):
    loudness = 1.0
    for dim, parts in cuts:
        steps = jax.random.uniform(jax.random.fold_in(jax.random.fold_in(rng, 6), dim), (parts,), jnp.float32, smallest / len(cuts), high / len(cuts))
        loudness = loudness * jnp.repeat(jnp.exp(steps), shape[dim] // parts).reshape((-1,) + (1,) * (len(shape) - 1 - dim))
    return loudness


def scatter_about(key, shape, width, limit, cuts=(), kind=jnp.bfloat16):
    loudness = shard_levels(key, shape, cuts, -0.22, 0.18) if cuts else 1.0
    values = jax.random.normal(key, shape, jnp.float32) * width * loudness
    return jnp.minimum(jnp.maximum(values, -limit), limit).astype(kind)


def setup_inputs(seed: int = 0) -> dict:
    streams_of = jax.random.split(jax.random.key(seed), 7)
    return {
        "query": draw_query(jax.random.fold_in(streams_of[6], 71), 0),
        "keys": draw_keys(jax.random.fold_in(streams_of[6], 71), 0),
        "values": scatter_about(streams_of[2], (TOKENS, D), 1.0, 6.0, ((0, 32), (1, 4))),
        "lr_code": draw_lr_code(jax.random.fold_in(streams_of[6], 71), 0),
        "fast_weights": scatter_about(streams_of[4], (FHEADS, 3, FW, FW), FW ** -0.5, 0.25, ((0, 4),)),
        "out_weight": scatter_about(streams_of[5], (D, D), D ** -0.5, 0.09375, ((0, 4),)),
    }


base_rate = 0.05

def attention(query, keys, values):
    head_count = D // HEAD_DIM
    block_rows = math.gcd(512, TOKENS)
    q_all = query.reshape(TOKENS, head_count, HEAD_DIM)
    zero_pad = jnp.zeros((WINDOW, head_count, HEAD_DIM), keys.dtype)
    key_all = jnp.concatenate([zero_pad, keys.reshape(TOKENS, head_count, HEAD_DIM)], 0)
    val_all = jnp.concatenate([zero_pad, values.reshape(TOKENS, head_count, HEAD_DIM)], 0)
    score_scale = 1.0 / math.sqrt(HEAD_DIM)

    def one_block(blk_index):
        row_start = blk_index * block_rows
        q_block = lax.dynamic_slice_in_dim(q_all, row_start, block_rows, 0).astype(jnp.float32)
        k_block = lax.dynamic_slice_in_dim(key_all, row_start, block_rows + WINDOW, 0).astype(jnp.float32)
        v_block = lax.dynamic_slice_in_dim(val_all, row_start, block_rows + WINDOW, 0).astype(jnp.float32)
        scores = jnp.einsum('qhd,khd->hqk', q_block, k_block) * score_scale
        q_pos = row_start + jnp.arange(block_rows, dtype=jnp.int32)[:, None]
        k_pos = row_start - WINDOW + jnp.arange(block_rows + WINDOW, dtype=jnp.int32)[None, :]
        live = (k_pos <= q_pos) & (k_pos > q_pos - WINDOW) & (k_pos >= 0)
        scores = jnp.where(live[None], scores, jnp.float32(-1e+30))
        top_score = lax.optimization_barrier(jnp.max(scores, axis=-1, keepdims=True))
        exps = jnp.exp(scores - top_score)
        probs = (exps / lax.optimization_barrier(jnp.sum(exps, axis=-1, keepdims=True))).astype(jnp.bfloat16)
        head_out = jnp.einsum('hqk,khd->qhd', probs.astype(jnp.float32), v_block)
        return head_out.reshape(block_rows, D)
    blocks_out = lax.map(one_block, jnp.arange(TOKENS // block_rows, dtype=jnp.int32))
    return blocks_out.reshape(TOKENS, D)

def contract_rows(left, right):
    return lax.dot_general(left, right, (((0,), (0,)), ((), ())), preferred_element_type=jnp.float32)

def train_head(keys_h, values_h, rate_h, weights):
    gate_in = jnp.dot(keys_h, weights[0], preferred_element_type=jnp.float32)
    up_in = jnp.dot(keys_h, weights[1], preferred_element_type=jnp.float32)
    sigmoid_val = jax.nn.sigmoid(gate_in)
    gated_act = (gate_in * sigmoid_val * up_in).astype(jnp.bfloat16)
    pushed = (rate_h[:, None] * values_h.astype(jnp.float32)).astype(jnp.bfloat16)
    back_grad = lax.dot_general(pushed, weights[2], (((1,), (1,)), ((), ())), preferred_element_type=jnp.float32)
    d_gate = (back_grad * up_in * sigmoid_val * (1.0 + gate_in * (1.0 - sigmoid_val))).astype(jnp.bfloat16)
    d_up = (back_grad * gate_in * sigmoid_val).astype(jnp.bfloat16)
    return jnp.stack([contract_rows(keys_h, d_gate), contract_rows(keys_h, d_up), contract_rows(gated_act, pushed)])

def renorm(start_w, grad_pull, step_size):
    base_w = start_w.astype(jnp.float32)
    updated = base_w + step_size[:, None, None, None] * grad_pull
    old_norm = jnp.sqrt(lax.optimization_barrier(jnp.sum(base_w * base_w, axis=2, keepdims=True)) + 1e-06)
    new_norm = jnp.sqrt(lax.optimization_barrier(jnp.sum(updated * updated, axis=2, keepdims=True)) + 1e-06)
    return (updated * (old_norm / new_norm)).astype(jnp.bfloat16)

def apply_head(query_h, weights):
    gate_in = jnp.dot(query_h, weights[0], preferred_element_type=jnp.float32)
    up_in = jnp.dot(query_h, weights[1], preferred_element_type=jnp.float32)
    gated_q = (gate_in * jax.nn.sigmoid(gate_in) * up_in).astype(jnp.bfloat16)
    head_out = jnp.dot(gated_q, weights[2], preferred_element_type=jnp.float32)
    return head_out * lax.rsqrt(lax.optimization_barrier(jnp.mean(head_out * head_out, axis=-1, keepdims=True)) + 1e-06)

def reference(query, keys, values, lr_code, fast_weights, out_weight):
    attended = attention(query, keys, values)
    rate = lr_code.astype(jnp.float32) * 2.0 ** (-14)
    step_size = base_rate / (math.sqrt(TOKENS) * (lax.optimization_barrier(jnp.sum(rate, axis=0)) / TOKENS))
    grad_pull = jnp.stack([train_head(keys[:, head_idx * FW:(head_idx + 1) * FW], values[:, head_idx * FW:(head_idx + 1) * FW], rate[:, head_idx], fast_weights[head_idx]) for head_idx in range(FHEADS)])
    new_weights = renorm(fast_weights, grad_pull, step_size)
    fast_out = jnp.concatenate([apply_head(query[:, head_idx * FW:(head_idx + 1) * FW], new_weights[head_idx]) for head_idx in range(FHEADS)], 1)
    merged = (attended + fast_out).astype(jnp.bfloat16)
    group_width = D // N_HEAD
    layer_sum = jnp.zeros((TOKENS, D), jnp.float32)
    for group_idx in range(N_HEAD):
        part_out = jnp.dot(merged[:, group_idx * group_width:(group_idx + 1) * group_width], out_weight[group_idx * group_width:(group_idx + 1) * group_width], preferred_element_type=jnp.float32).astype(jnp.bfloat16)
        layer_sum = layer_sum + part_out.astype(jnp.float32)
    return (layer_sum.astype(jnp.bfloat16), new_weights)
```

```python
import math

import jax
import jax.numpy as jnp
from jax import lax
from jax.experimental import pallas as pl
from jax.experimental.pallas import tpu as pltpu
from jax.sharding import PartitionSpec as P

FW = 512
HEAD_DIM = 128
WINDOW = 256
BASE_RATE = 0.05
BLOCK = 256
F32 = jnp.float32
BF16 = jnp.bfloat16
MESH = pl.DeviceIdType.MESH
MIB = 1024 * 1024


def dot(left, right, left_dim=1, right_dim=0):
    return lax.dot_general(
        left, right, (((left_dim,), (right_dim,)), ((), ())), preferred_element_type=F32
    )


def sigmoid(x):
    return 0.5 * jnp.tanh(0.5 * x) + 0.5


RIM_K, RIM_V, CORE_G, CORE_R = 0, 1, 2, 3
X_A, X_B, X_R = 3, 6, 9
Y_A, Y_B, Y_R = 12, 15, 18
GY_A, GY_B, GX_A, GX_B = 21, 24, 27, 30
CORE_P = 34
COPIES = 35
RING = 4


def update_kernel(
    q_hbm, k_hbm, v_hbm, code_ref, fw_hbm,
    att_ref, pull_hbm, rate_ref,
    q_buf, k_buf, v_buf, fw_buf, d_buf, gated_buf, pushed_buf,
    grad_out, grad_in, grad_sum, in_xa, in_xb, sum_a, sum_b, in_ya, in_yb,
    pull_buf, rate_out, rate_in, load_sem, store_sem, send_sem, recv_sem,
):
    ctx = lax.axis_index("ctx")
    core = lax.rem(ctx, 2)
    chip = lax.div(ctx, 2)
    y = lax.rem(chip, RING)
    x = lax.div(chip, RING)
    contexts = lax.axis_size("ctx")
    rows = k_hbm.shape[0]
    blocks = rows // BLOCK
    part = in_xa.shape[1]
    piece = in_ya.shape[1]
    half = grad_sum.shape[0] // 2

    def at(xx, yy, cc):
        return (xx * RING + yy) * 2 + cc

    partner = at(x, y, 1 - core)
    follower = lax.rem(ctx + 1, contexts)
    leader = lax.rem(ctx + contexts - 1, contexts)
    x_peer = [None] + [at(lax.rem(x + d, RING), y, core) for d in range(1, RING)]
    y_peer = [None] + [at(x, lax.rem(y + d, RING), core) for d in range(1, RING)]

    def load(src, dst, index):
        return pltpu.make_async_copy(src, dst, load_sem.at[index])

    first, second = 1 - core, core

    def lanes(head):
        return pl.ds(pl.multiple_of(head * FW, FW), FW)

    loads = {}
    for order, head in enumerate((first, second)):
        loads["w", order] = load(fw_hbm.at[head], fw_buf.at[head], 4 * order)
        loads["k", order] = load(
            k_hbm.at[:, lanes(head)], k_buf.at[head, pl.ds(WINDOW, rows)], 4 * order + 1
        )
        loads["v", order] = load(
            v_hbm.at[:, lanes(head)], v_buf.at[head, pl.ds(WINDOW, rows)], 4 * order + 2
        )
        loads["q", order] = load(q_hbm.at[:, lanes(head)], q_buf.at[head], 4 * order + 3)
    for name in ("w", "k", "v"):
        for order in range(2):
            loads[name, order].start()

    barrier = pltpu.get_barrier_semaphore()
    peers = [follower, leader] + x_peer[1:] + y_peer[1:]
    for peer in peers:
        pl.semaphore_signal(barrier, inc=1, device_id={"ctx": peer}, device_id_type=MESH)
    pl.semaphore_wait(barrier, len(peers))

    def remote(src, dst, index, peer):
        return pltpu.make_async_remote_copy(
            src_ref=src, dst_ref=dst, send_sem=send_sem.at[index], recv_sem=recv_sem.at[index],
            device_id={"ctx": peer}, device_id_type=MESH,
        )

    sent = []

    def send(copy):
        copy.start()
        sent.append(copy)
        return copy

    for order in range(2):
        loads["k", order].wait()
        loads["v", order].wait()
    for order in range(2):
        loads["q", order].start()
    rim = [
        send(remote(k_buf.at[:, pl.ds(rows, WINDOW)], k_buf.at[:, pl.ds(0, WINDOW)], RIM_K, follower)),
        send(remote(v_buf.at[:, pl.ds(rows, WINDOW)], v_buf.at[:, pl.ds(0, WINDOW)], RIM_V, follower)),
    ]

    rate = code_ref[...].astype(F32) * 2.0 ** (-14)
    rate_out[0] = jnp.broadcast_to(jnp.sum(rate, axis=1, keepdims=True), rate_out.shape[1:])
    core_rate = send(remote(rate_out.at[0], rate_in.at[0], CORE_R, partner))

    def train(head):
        def tokens(t, carry):
            start = pl.multiple_of(t * BLOCK, BLOCK)
            k_rows = k_buf[head, pl.ds(start + WINDOW, BLOCK)]
            v_rows = v_buf[head, pl.ds(start + WINDOW, BLOCK)].astype(F32)
            code_row = code_ref[pl.ds(head, 1), pl.ds(start, BLOCK)].astype(F32) * 2.0 ** (-14)
            column = jnp.transpose(jnp.broadcast_to(code_row, (8, BLOCK)))[:, 0:1]
            pushed = (column * v_rows).astype(BF16)
            gate_in = dot(k_rows, fw_buf[head, 0])
            up_in = dot(k_rows, fw_buf[head, 1])
            back = dot(pushed, fw_buf[head, 2], 1, 1)
            s = sigmoid(gate_in)
            gs = gate_in * s
            here = pl.ds(start, BLOCK)
            pushed_buf[here] = pushed
            gated_buf[here] = (gs * up_in).astype(BF16)
            d_buf[here, 0:FW] = (back * up_in * (s * (1.0 + gate_in * (1.0 - s)))).astype(BF16)
            d_buf[here, FW : 2 * FW] = (back * gs).astype(BF16)
            return carry

        lax.fori_loop(0, blocks, tokens, 0)

    def pulls(head, put):
        for i in range(FW // BLOCK):
            cols = pl.ds(i * BLOCK, BLOCK)
            k_cols = k_buf[head, pl.ds(WINDOW, rows), cols]
            both = dot(k_cols, d_buf[...], 0, 0)
            put(pl.ds(i * BLOCK, BLOCK), both[:, 0:FW])
            put(pl.ds(FW + i * BLOCK, BLOCK), both[:, FW : 2 * FW])
            put(pl.ds(2 * FW + i * BLOCK, BLOCK), dot(gated_buf[:, cols], pushed_buf[...], 0, 0))

    def put_out(where, value):
        grad_out[where] = value.astype(BF16)

    def put_sum(where, value):
        grad_sum[where] = (value + grad_in[where].astype(F32)).astype(BF16)

    loads["w", 0].wait()
    train(first)
    pulls(first, put_out)
    core_grad = send(remote(grad_out, grad_in, CORE_G, partner))
    loads["w", 1].wait()
    train(second)
    core_rate.wait_recv()
    rate_out[1] = rate_out[0] + rate_in[0]
    core_grad.wait_recv()
    pulls(second, put_sum)

    def aligned(start, size):
        return pl.ds(pl.multiple_of(start, 16), size)

    def ring_to(index):
        return lax.rem(index, RING)

    out_x = []
    for d in range(1, RING):
        out_x.append(send(remote(
            grad_sum.at[aligned(ring_to(x + d) * part, part)], in_xa.at[d - 1], X_A + d, x_peer[d])))
        out_x.append(send(remote(
            grad_sum.at[aligned(half + ring_to(y + d) * part, part)], in_xb.at[d - 1], X_B + d, y_peer[d])))
        out_x.append(send(remote(rate_out.at[1], rate_in.at[d], X_R + d, x_peer[d])))

    for copy in rim:
        copy.wait_recv()
    for order in range(2):
        loads["q", order].wait()

    row_id = lax.broadcasted_iota(jnp.int32, (BLOCK, BLOCK), 0)
    col_id = lax.broadcasted_iota(jnp.int32, (BLOCK, BLOCK), 1)
    scale = math.log2(math.e) / math.sqrt(HEAD_DIM)

    def attend(unit, carry):
        head = lax.div(unit, blocks)
        block = lax.rem(unit, blocks)
        start = pl.multiple_of(block * BLOCK, BLOCK)
        unseen = jnp.where((ctx == 0) & (block == 0), -1e30, 0.0).astype(F32)
        causal = col_id <= row_id
        for j in range(FW // HEAD_DIM):
            cols = pl.ds(j * HEAD_DIM, HEAD_DIM)
            q_rows = q_buf[head, pl.ds(start, BLOCK), cols]
            scores = dot(q_rows, k_buf[head, pl.ds(start, 2 * BLOCK), cols], 1, 1)
            live = jnp.where(causal, scores[:, BLOCK:], scores[:, :BLOCK] + unseen)
            top = jnp.max(live, axis=1, keepdims=True)
            exps = jnp.exp2((live - top) * scale)
            old = jnp.where(causal, 0.0, exps).astype(BF16)
            new = jnp.where(causal, exps, 0.0).astype(BF16)
            ones = jnp.ones((BLOCK, HEAD_DIM), BF16)
            v_old = jnp.concatenate([v_buf[head, pl.ds(start, BLOCK), cols], ones], 1)
            v_new = jnp.concatenate([v_buf[head, pl.ds(start + BLOCK, BLOCK), cols], ones], 1)
            both = dot(old, v_old) + dot(new, v_new)
            att_ref[head, pl.ds(start, BLOCK), cols] = (
                both[:, :HEAD_DIM] / both[:, HEAD_DIM:]
            ).astype(BF16)
        return carry

    units = 2 * blocks
    lax.fori_loop(0, units // 2, attend, 0)

    for copy in out_x:
        copy.wait_recv()

    def total(own, others):
        value = own.astype(F32)
        for i in range(RING - 1):
            value = value + others[i].astype(F32)
        return value

    sum_a[...] = total(grad_sum[aligned(x * part, part)], in_xa).astype(BF16)
    sum_b[...] = total(grad_sum[aligned(half + y * part, part)], in_xb).astype(BF16)
    rate_out[2] = rate_out[1] + rate_in[1] + rate_in[2] + rate_in[3]

    out_y = []
    for d in range(1, RING):
        out_y.append(send(remote(
            sum_a.at[aligned(ring_to(y + d) * piece, piece)], in_ya.at[d - 1], Y_A + d, y_peer[d])))
        out_y.append(send(remote(
            sum_b.at[aligned(ring_to(x + d) * piece, piece)], in_yb.at[d - 1], Y_B + d, x_peer[d])))
        out_y.append(send(remote(rate_out.at[2], rate_in.at[RING - 1 + d], Y_R + d, y_peer[d])))
    lax.fori_loop(units // 2, units // 2 + 1, attend, 0)
    for copy in out_y:
        copy.wait_recv()
    own_a = aligned(x * part + y * piece, piece)
    own_b = aligned(half + y * part + x * piece, piece)
    pull_buf[core, own_a] = total(sum_a[aligned(y * piece, piece)], in_ya).astype(BF16)
    pull_buf[core, own_b] = total(sum_b[aligned(x * piece, piece)], in_yb).astype(BF16)
    rate_ref[...] = rate_out[2] + rate_in[4] + rate_in[5] + rate_in[6]

    back_y = []
    for d in range(1, RING):
        mine_a, mine_b = pull_buf.at[core, own_a], pull_buf.at[core, own_b]
        back_y.append(send(remote(mine_a, mine_a, GY_A + d, y_peer[d])))
        back_y.append(send(remote(mine_b, mine_b, GY_B + d, x_peer[d])))
    lax.fori_loop(units // 2 + 1, units // 2 + 2, attend, 0)
    for copy in back_y:
        copy.wait_recv()

    back_x = []
    for d in range(1, RING):
        mine_a = pull_buf.at[core, aligned(x * part, part)]
        mine_b = pull_buf.at[core, aligned(half + y * part, part)]
        back_x.append(send(remote(mine_a, mine_a, GX_A + d, x_peer[d])))
        back_x.append(send(remote(mine_b, mine_b, GX_B + d, y_peer[d])))
    lax.fori_loop(units // 2 + 2, units, attend, 0)
    for copy in back_x:
        copy.wait_recv()

    across = send(remote(pull_buf.at[core], pull_buf.at[core], CORE_P, partner))
    store_own = pltpu.make_async_copy(pull_buf.at[core], pull_hbm.at[core], store_sem.at[0])
    store_own.start()
    across.wait_recv()
    store_other = pltpu.make_async_copy(pull_buf.at[1 - core], pull_hbm.at[1 - core], store_sem.at[1])
    store_other.start()
    for copy in sent:
        copy.wait_send()
    store_own.wait()
    store_other.wait()


def update(query, keys, values, code_t, fast_weights):
    rows, width = query.shape
    heads = width // FW
    pulled = 3 * FW
    part = pulled // 2 // RING
    piece = part // RING
    hbm = pl.BlockSpec(memory_space=pl.ANY)
    vmem = pl.BlockSpec(memory_space=pltpu.VMEM)
    return pl.pallas_call(
        update_kernel,
        out_shape=(
            jax.ShapeDtypeStruct((heads, rows, FW), BF16),
            jax.ShapeDtypeStruct((heads, pulled, FW), BF16),
            jax.ShapeDtypeStruct((heads, 128), F32),
        ),
        in_specs=[hbm, hbm, hbm, vmem, hbm],
        out_specs=(vmem, hbm, vmem),
        scratch_shapes=[
            pltpu.VMEM((heads, rows, FW), BF16),
            pltpu.VMEM((heads, rows + WINDOW, FW), BF16),
            pltpu.VMEM((heads, rows + WINDOW, FW), BF16),
            pltpu.VMEM((heads, 3, FW, FW), BF16),
            pltpu.VMEM((rows, 2 * FW), BF16),
            pltpu.VMEM((rows, FW), BF16),
            pltpu.VMEM((rows, FW), BF16),
            pltpu.VMEM((pulled, FW), BF16),
            pltpu.VMEM((pulled, FW), BF16),
            pltpu.VMEM((pulled, FW), BF16),
            pltpu.VMEM((RING - 1, part, FW), BF16),
            pltpu.VMEM((RING - 1, part, FW), BF16),
            pltpu.VMEM((part, FW), BF16),
            pltpu.VMEM((part, FW), BF16),
            pltpu.VMEM((RING - 1, piece, FW), BF16),
            pltpu.VMEM((RING - 1, piece, FW), BF16),
            pltpu.VMEM((heads, pulled, FW), BF16),
            pltpu.VMEM((3, heads, 128), F32),
            pltpu.VMEM((7, heads, 128), F32),
            pltpu.SemaphoreType.DMA((8,)),
            pltpu.SemaphoreType.DMA((2,)),
            pltpu.SemaphoreType.DMA((COPIES,)),
            pltpu.SemaphoreType.DMA((COPIES,)),
        ],
        compiler_params=pltpu.CompilerParams(
            collective_id=0, has_side_effects=True, vmem_limit_bytes=56 * MIB
        ),
        name="update",
    )(query, keys, values, code_t, fast_weights)


def renorm_kernel(tokens_all, rate_ref, pull_ref, fw_ref, new_ref):
    head = lax.div(pl.program_id(0), 3)
    rate_sum = jnp.where(head == 0, rate_ref[0:1, 0:1], rate_ref[1:2, 0:1])
    step = BASE_RATE / (math.sqrt(tokens_all) * (rate_sum / tokens_all))
    base = fw_ref[0].astype(F32)
    updated = base + step * pull_ref[0].astype(F32)
    old = jnp.sqrt(jnp.sum(base * base, axis=0, keepdims=True) + 1e-06)
    new = jnp.sqrt(jnp.sum(updated * updated, axis=0, keepdims=True) + 1e-06)
    new_ref[0] = (updated * (old / new)).astype(BF16)


def renorm(rate_sum, pull, fast_weights, tokens_all):
    count = pull.shape[0]
    matrix = pl.BlockSpec((1, FW, FW), lambda i: (i, 0, 0))

    def kernel(*refs):
        renorm_kernel(tokens_all, *refs)

    return pl.pallas_call(
        kernel,
        grid=(count,),
        out_shape=jax.ShapeDtypeStruct((count, FW, FW), BF16),
        in_specs=[pl.BlockSpec(rate_sum.shape, lambda i: (0, 0)), matrix, matrix],
        out_specs=matrix,
        name="renorm",
    )(rate_sum, pull, fast_weights)


SUBS = 4
HALF = 512


def project_kernel(
    q_hbm, att_hbm, nw_hbm, w_hbm, out_ref,
    q_buf, att_buf, nw_buf, w_buf, merged, out_buf, in_buf,
    load_sem, send_sem, recv_sem,
):
    me = lax.axis_index("head")
    n = lax.axis_size("head")
    ahead, behind = lax.rem(me + 1, n), lax.rem(me + n - 1, n)
    targets = (ahead, behind)
    rows = out_ref.shape[0]
    sub_rows = rows // SUBS
    heads = att_buf.shape[0]

    loads = []

    def load(src, dst):
        copy = pltpu.make_async_copy(src, dst, load_sem.at[len(loads)])
        copy.start()
        loads.append(copy)
        return copy

    nw_load = load(nw_hbm, nw_buf)
    first_loads = [nw_load]
    for h in range(heads):
        first_loads.append(load(q_hbm.at[:, pl.ds(h * FW, FW)], q_buf.at[h]))
    first_loads.append(load(att_hbm, att_buf))
    w_loads = {}
    for step in range(n):
        for way in range(2):
            dest = lax.rem(me + n - 1 - step, n) if way == 0 else lax.rem(me + 1 + step, n)
            start = pl.multiple_of(dest * (2 * HALF) + way * HALF, HALF)
            w_loads[step, way] = load(w_hbm.at[:, pl.ds(start, HALF)], w_buf.at[2 * step + way])

    barrier = pltpu.get_barrier_semaphore()
    for peer in targets:
        pl.semaphore_signal(barrier, inc=1, device_id={"head": peer}, device_id_type=MESH)
    pl.semaphore_wait(barrier, 2)

    def hop(step, sub, way):
        index = (step * SUBS + sub) * 2 + way
        return pltpu.make_async_remote_copy(
            src_ref=out_buf.at[step, sub, way], dst_ref=in_buf.at[step, sub, way],
            send_sem=send_sem.at[index], recv_sem=recv_sem.at[index],
            device_id={"head": targets[way]}, device_id_type=MESH,
        )

    for copy in first_loads:
        copy.wait()
    for way in range(2):
        w_loads[0, way].wait()

    def partial(step, sub, way):
        here = pl.ds(pl.multiple_of(sub * sub_rows, sub_rows), sub_rows)
        return dot(merged[here], w_buf[2 * step + way])

    def opening(sub, carry):
        here = pl.ds(pl.multiple_of(sub * sub_rows, sub_rows), sub_rows)
        for h in range(heads):
            q_rows = q_buf[h, here]
            gate_in = dot(q_rows, nw_buf[h, 0])
            up_in = dot(q_rows, nw_buf[h, 1])
            gated = (gate_in * sigmoid(gate_in) * up_in).astype(BF16)
            value = dot(gated, nw_buf[h, 2])
            norm = lax.rsqrt(jnp.mean(value * value, axis=1, keepdims=True) + 1e-06)
            merged[here, h * FW : (h + 1) * FW] = (
                att_buf[h, here].astype(F32) + value * norm
            ).astype(BF16)
        for way in range(2):
            out_buf[0, sub, way] = partial(0, sub, way).astype(BF16)
            hop(0, sub, way).start()
        return carry

    lax.fori_loop(0, SUBS, opening, 0)

    for step in range(1, n):
        for way in range(2):
            w_loads[step, way].wait()

        def middle(sub, carry, step=step):
            for way in range(2):
                mine = partial(step, sub, way)
                hop(step - 1, sub, way).wait_recv()
                value = (mine + in_buf[step - 1, sub, way].astype(F32)).astype(BF16)
                if step < n - 1:
                    out_buf[step, sub, way] = value
                    hop(step, sub, way).start()
                else:
                    here = pl.ds(pl.multiple_of(sub * sub_rows, sub_rows), sub_rows)
                    out_ref[here, way * HALF : (way + 1) * HALF] = value
            return carry

        lax.fori_loop(0, SUBS, middle, 0)

    for step in range(n - 1):

        def drain(sub, carry, step=step):
            for way in range(2):
                hop(step, sub, way).wait_send()
            return carry

        lax.fori_loop(0, SUBS, drain, 0)


def project(query, attended, new_weights, out_weight, n):
    rows, width = query.shape
    heads = width // FW
    sub_rows = rows // SUBS
    hbm = pl.BlockSpec(memory_space=pl.ANY)
    return pl.pallas_call(
        project_kernel,
        out_shape=jax.ShapeDtypeStruct((rows, 2 * HALF), BF16),
        in_specs=[hbm] * 4,
        out_specs=pl.BlockSpec(memory_space=pltpu.VMEM),
        scratch_shapes=[
            pltpu.VMEM((heads, rows, FW), BF16),
            pltpu.VMEM((heads, rows, FW), BF16),
            pltpu.VMEM((heads, 3, FW, FW), BF16),
            pltpu.VMEM((2 * n, width, HALF), BF16),
            pltpu.VMEM((rows, width), BF16),
            pltpu.VMEM((n - 1, SUBS, 2, sub_rows, HALF), BF16),
            pltpu.VMEM((n - 1, SUBS, 2, sub_rows, HALF), BF16),
            pltpu.SemaphoreType.DMA((2 * n + heads + 2,)),
            pltpu.SemaphoreType.DMA(((n - 1) * SUBS * 2,)),
            pltpu.SemaphoreType.DMA(((n - 1) * SUBS * 2,)),
        ],
        compiler_params=pltpu.CompilerParams(
            collective_id=1, has_side_effects=True, vmem_limit_bytes=56 * MIB
        ),
        name="project",
    )(query, attended, new_weights, out_weight)


def shards(query, keys, values, lr_code, fast_weights, out_weight):
    heads = fast_weights.shape[0]
    tokens_all = query.shape[0] * lax.axis_size("ctx")
    attended, pull, rate_sum = update(query, keys, values, lr_code.T, fast_weights)
    new_weights = renorm(
        rate_sum, pull.reshape(heads * 3, FW, FW), fast_weights.reshape(heads * 3, FW, FW), tokens_all
    ).reshape(heads, 3, FW, FW)
    layer_out = project(query, attended, new_weights, out_weight, lax.axis_size("head"))
    return (layer_out, new_weights)


def solution(mesh):
    placed = (
        P("ctx", "head"),
        P("ctx", "head"),
        P("ctx", "head"),
        P("ctx", "head"),
        P("head", None, None, None),
        P("head", None),
    )
    return jax.shard_map(
        shards,
        mesh=mesh,
        in_specs=placed,
        out_specs=(P("ctx", "head"), P("head", None, None, None)),
        check_vma=False,
    )
```

```python
import math

import jax
import jax.numpy as jnp
from jax import lax
from jax.experimental import pallas as pl
from jax.experimental.pallas import tpu as pltpu
from jax.sharding import PartitionSpec as P

FW = 512
HEAD_DIM = 128
WINDOW = 256
BASE_RATE = 0.05
BLOCK = 256
F32 = jnp.float32
BF16 = jnp.bfloat16
MESH = pl.DeviceIdType.MESH
MIB = 1024 * 1024


def dot(left, right, left_dim=1, right_dim=0):
    return lax.dot_general(
        left, right, (((left_dim,), (right_dim,)), ((), ())), preferred_element_type=F32
    )


def sigmoid(x):
    return 0.5 * jnp.tanh(0.5 * x) + 0.5


RIM_K, RIM_V, CORE_G, CORE_R = 0, 1, 2, 3
X_A, X_B, X_R = 3, 6, 9
Y_A, Y_B, Y_R = 12, 15, 18
GY_A, GY_B, GX_A, GX_B = 21, 24, 27, 30
CORE_P = 34
COPIES = 35
RING = 4
SUBS = 4
HALF = 512


def layer_kernel(
    q_hbm, k_hbm, v_hbm, code_ref, fw_hbm, w_hbm,
    out_hbm, new_hbm,
    q_buf, k_buf, v_buf, fw_buf, base_buf, d_buf, gated_buf, pushed_buf,
    grad_out, grad_in, grad_sum, in_xa, in_xb, sum_a, sum_b, in_ya, in_yb,
    new_buf, rate_out, rate_in, att_buf, w_buf, merged, ring_out, ring_in, out_buf,
    load_sem, w_sem, store_sem, send_sem, recv_sem, ring_send, ring_recv,
):
    ctx = lax.axis_index("ctx")
    me = lax.axis_index("head")
    core = lax.rem(ctx, 2)
    chip = lax.div(ctx, 2)
    y = lax.rem(chip, RING)
    x = lax.div(chip, RING)
    contexts = lax.axis_size("ctx")
    groups = lax.axis_size("head")
    rows = k_hbm.shape[0]
    tokens_all = rows * contexts
    blocks = rows // BLOCK
    part = in_xa.shape[1]
    piece = in_ya.shape[1]
    half = grad_sum.shape[0] // 2
    heads = fw_buf.shape[0]

    def at(xx, yy, cc):
        return (xx * RING + yy) * 2 + cc

    partner = at(x, y, 1 - core)
    follower = lax.rem(ctx + 1, contexts)
    leader = lax.rem(ctx + contexts - 1, contexts)
    x_peer = [None] + [at(lax.rem(x + d, RING), y, core) for d in range(1, RING)]
    y_peer = [None] + [at(x, lax.rem(y + d, RING), core) for d in range(1, RING)]
    ring_peer = (lax.rem(me + 1, groups), lax.rem(me + groups - 1, groups))

    def load(src, dst, index):
        return pltpu.make_async_copy(src, dst, load_sem.at[index])

    first, second = 1 - core, core

    def lanes(head):
        return pl.ds(pl.multiple_of(head * FW, FW), FW)

    loads = {}
    for order, head in enumerate((first, second)):
        loads["w", order] = load(fw_hbm.at[head], fw_buf.at[head], 4 * order)
        loads["k", order] = load(
            k_hbm.at[:, lanes(head)], k_buf.at[head, pl.ds(WINDOW, rows)], 4 * order + 1
        )
        loads["v", order] = load(
            v_hbm.at[:, lanes(head)], v_buf.at[head, pl.ds(WINDOW, rows)], 4 * order + 2
        )
        loads["q", order] = load(q_hbm.at[:, lanes(head)], q_buf.at[head], 4 * order + 3)
    w_loads = {}
    for step in range(RING):
        for way in range(2):
            dest = lax.rem(me + groups - 1 - step, groups) if way == 0 else lax.rem(me + 1 + step, groups)
            start = pl.multiple_of(dest * (2 * HALF) + way * HALF, HALF)
            index = 2 * step + way
            w_loads[step, way] = pltpu.make_async_copy(
                w_hbm.at[:, pl.ds(start, HALF)], w_buf.at[index], w_sem.at[index]
            )
    for order in range(2):
        for name in ("w", "k", "v"):
            loads[name, order].start()

    barrier = pltpu.get_barrier_semaphore()
    ctx_peers = [follower, leader] + x_peer[1:] + y_peer[1:]
    for peer in ctx_peers:
        pl.semaphore_signal(barrier, inc=1, device_id={"ctx": peer}, device_id_type=MESH)
    for peer in ring_peer:
        pl.semaphore_signal(barrier, inc=1, device_id={"head": peer}, device_id_type=MESH)

    def remote(src, dst, index, peer):
        return pltpu.make_async_remote_copy(
            src_ref=src, dst_ref=dst, send_sem=send_sem.at[index], recv_sem=recv_sem.at[index],
            device_id={"ctx": peer}, device_id_type=MESH,
        )

    sent = []

    def send(copy):
        copy.start()
        sent.append(copy)
        return copy

    def train(head):
        def tokens(t, carry):
            start = pl.multiple_of(t * BLOCK, BLOCK)
            k_rows = k_buf[head, pl.ds(start + WINDOW, BLOCK)]
            v_rows = v_buf[head, pl.ds(start + WINDOW, BLOCK)].astype(F32)
            code_row = code_ref[pl.ds(head, 1), pl.ds(start, BLOCK)].astype(F32) * 2.0 ** (-14)
            column = jnp.transpose(jnp.broadcast_to(code_row, (8, BLOCK)))[:, 0:1]
            pushed = (column * v_rows).astype(BF16)
            gate_in = dot(k_rows, fw_buf[head, 0])
            up_in = dot(k_rows, fw_buf[head, 1])
            back = dot(pushed, fw_buf[head, 2], 1, 1)
            s = sigmoid(gate_in)
            gs = gate_in * s
            here = pl.ds(start, BLOCK)
            pushed_buf[here] = pushed
            gated_buf[here] = (gs * up_in).astype(BF16)
            d_buf[here, 0:FW] = (back * up_in * (s * (1.0 + gate_in * (1.0 - s)))).astype(BF16)
            d_buf[here, FW : 2 * FW] = (back * gs).astype(BF16)
            return carry

        lax.fori_loop(0, blocks, tokens, 0)

    def pulls(head, put):
        k_own = k_buf.at[head, pl.ds(WINDOW, rows)]
        for i in range(2 * FW // BLOCK):
            cols = pl.ds(i * BLOCK, BLOCK)
            put(cols, dot(d_buf[:, cols], k_own[...], 0, 0))
        for i in range(FW // BLOCK):
            cols = pl.ds(i * BLOCK, BLOCK)
            put(pl.ds(2 * FW + i * BLOCK, BLOCK), dot(pushed_buf[:, cols], gated_buf[...], 0, 0))

    def put_out(where, value):
        grad_out[where] = value.astype(BF16)

    def put_sum(where, value):
        grad_sum[where] = (value + grad_in[where].astype(F32)).astype(BF16)

    for name in ("w", "k", "v"):
        loads[name, 0].wait()
    train(first)
    for name in ("w", "k", "v"):
        loads[name, 1].wait()
    for order in range(2):
        loads["q", order].start()
    for copy in w_loads.values():
        copy.start()
    pl.semaphore_wait(barrier, len(ctx_peers) + len(ring_peer))
    rim = [
        send(remote(k_buf.at[:, pl.ds(rows, WINDOW)], k_buf.at[:, pl.ds(0, WINDOW)], RIM_K, follower)),
        send(remote(v_buf.at[:, pl.ds(rows, WINDOW)], v_buf.at[:, pl.ds(0, WINDOW)], RIM_V, follower)),
    ]
    pulls(first, put_out)
    core_grad = send(remote(grad_out, grad_in, CORE_G, partner))
    rate = code_ref[...].astype(F32) * 2.0 ** (-14)
    rate_out[0] = jnp.broadcast_to(jnp.sum(rate, axis=1, keepdims=True), rate_out.shape[1:])
    core_rate = send(remote(rate_out.at[0], rate_in.at[0], CORE_R, partner))
    train(second)
    core_rate.wait_recv()
    rate_out[1] = rate_out[0] + rate_in[0]
    core_grad.wait_recv()
    pulls(second, put_sum)

    def aligned(start, size):
        return pl.ds(pl.multiple_of(start, 16), size)

    def ring_to(index):
        return lax.rem(index, RING)

    out_x = []
    for d in range(1, RING):
        out_x.append(send(remote(
            grad_sum.at[aligned(ring_to(x + d) * part, part)], in_xa.at[d - 1], X_A + d, x_peer[d])))
        out_x.append(send(remote(
            grad_sum.at[aligned(half + ring_to(y + d) * part, part)], in_xb.at[d - 1], X_B + d, y_peer[d])))
        out_x.append(send(remote(rate_out.at[1], rate_in.at[d], X_R + d, x_peer[d])))

    for m in range(3):
        base_buf[m * FW : (m + 1) * FW] = jnp.transpose(fw_buf[core, m])
    for copy in rim:
        copy.wait_recv()
    for order in range(2):
        loads["q", order].wait()

    row_id = lax.broadcasted_iota(jnp.int32, (BLOCK, BLOCK), 0)
    col_id = lax.broadcasted_iota(jnp.int32, (BLOCK, BLOCK), 1)
    scale = math.log2(math.e) / math.sqrt(HEAD_DIM)

    def attend(unit, carry):
        head = lax.div(unit, blocks)
        block = lax.rem(unit, blocks)
        start = pl.multiple_of(block * BLOCK, BLOCK)
        unseen = jnp.where((ctx == 0) & (block == 0), -1e30, 0.0).astype(F32)
        causal = col_id <= row_id
        for j in range(FW // HEAD_DIM):
            cols = pl.ds(j * HEAD_DIM, HEAD_DIM)
            q_rows = q_buf[head, pl.ds(start, BLOCK), cols]
            scores = dot(q_rows, k_buf[head, pl.ds(start, 2 * BLOCK), cols], 1, 1)
            live = jnp.where(causal, scores[:, BLOCK:], scores[:, :BLOCK] + unseen)
            top = jnp.max(live, axis=1, keepdims=True)
            exps = jnp.exp2((live - top) * scale)
            old = jnp.where(causal, 0.0, exps).astype(BF16)
            new = jnp.where(causal, exps, 0.0).astype(BF16)
            ones = jnp.ones((BLOCK, HEAD_DIM), BF16)
            v_old = jnp.concatenate([v_buf[head, pl.ds(start, BLOCK), cols], ones], 1)
            v_new = jnp.concatenate([v_buf[head, pl.ds(start + BLOCK, BLOCK), cols], ones], 1)
            both = dot(old, v_old) + dot(new, v_new)
            att_buf[head, pl.ds(start, BLOCK), cols] = (
                both[:, :HEAD_DIM] / both[:, HEAD_DIM:]
            ).astype(BF16)
        return carry

    units = 2 * blocks
    lax.fori_loop(0, units // 2, attend, 0)

    for copy in out_x:
        copy.wait_recv()

    def total(own, others):
        value = own.astype(F32)
        for i in range(RING - 1):
            value = value + others[i].astype(F32)
        return value

    sum_a[...] = total(grad_sum[aligned(x * part, part)], in_xa).astype(BF16)
    sum_b[...] = total(grad_sum[aligned(half + y * part, part)], in_xb).astype(BF16)
    rate_out[2] = rate_out[1] + rate_in[1] + rate_in[2] + rate_in[3]

    out_y = []
    for d in range(1, RING):
        out_y.append(send(remote(
            sum_a.at[aligned(ring_to(y + d) * piece, piece)], in_ya.at[d - 1], Y_A + d, y_peer[d])))
        out_y.append(send(remote(
            sum_b.at[aligned(ring_to(x + d) * piece, piece)], in_yb.at[d - 1], Y_B + d, x_peer[d])))
        out_y.append(send(remote(rate_out.at[2], rate_in.at[RING - 1 + d], Y_R + d, y_peer[d])))
    lax.fori_loop(units // 2, units // 2 + 1, attend, 0)
    for copy in out_y:
        copy.wait_recv()
    rate_out[3] = rate_out[2] + rate_in[4] + rate_in[5] + rate_in[6]
    step_size = BASE_RATE / (math.sqrt(tokens_all) * (rate_out[3, pl.ds(core, 1), 0:1] / tokens_all))

    def renorm(where, pull):
        base = base_buf[where].astype(F32)
        updated = base + step_size * pull
        old_norm = jnp.sqrt(jnp.sum(base * base, axis=1, keepdims=True) + 1e-06)
        new_norm = jnp.sqrt(jnp.sum(updated * updated, axis=1, keepdims=True) + 1e-06)
        new_buf[core, where] = (updated * (old_norm / new_norm)).astype(BF16)

    own_a = aligned(x * part + y * piece, piece)
    own_b = aligned(half + y * part + x * piece, piece)
    renorm(own_a, total(sum_a[aligned(y * piece, piece)], in_ya))
    renorm(own_b, total(sum_b[aligned(x * piece, piece)], in_yb))

    back_y = []
    for d in range(1, RING):
        mine_a, mine_b = new_buf.at[core, own_a], new_buf.at[core, own_b]
        back_y.append(send(remote(mine_a, mine_a, GY_A + d, y_peer[d])))
        back_y.append(send(remote(mine_b, mine_b, GY_B + d, x_peer[d])))
    lax.fori_loop(units // 2 + 1, units // 2 + 2, attend, 0)
    for copy in back_y:
        copy.wait_recv()

    back_x = []
    for d in range(1, RING):
        mine_a = new_buf.at[core, aligned(x * part, part)]
        mine_b = new_buf.at[core, aligned(half + y * part, part)]
        back_x.append(send(remote(mine_a, mine_a, GX_A + d, x_peer[d])))
        back_x.append(send(remote(mine_b, mine_b, GX_B + d, y_peer[d])))
    lax.fori_loop(units // 2 + 2, units, attend, 0)
    for copy in w_loads.values():
        copy.wait()
    for copy in back_x:
        copy.wait_recv()
    across = send(remote(new_buf.at[core], new_buf.at[core], CORE_P, partner))
    across.wait_recv()
    store_new = pltpu.make_async_copy(new_buf, new_hbm, store_sem.at[SUBS])
    store_new.start()

    sub_rows = rows // SUBS

    def hop(step, sub, way):
        index = (step * SUBS + sub) * 2 + way
        return pltpu.make_async_remote_copy(
            src_ref=ring_out.at[step, sub, way], dst_ref=ring_in.at[step, sub, way],
            send_sem=ring_send.at[index], recv_sem=ring_recv.at[index],
            device_id={"head": ring_peer[way]}, device_id_type=MESH,
        )

    def chunk(sub):
        return pl.ds(pl.multiple_of(sub * sub_rows, sub_rows), sub_rows)

    def partial(step, sub, way):
        return dot(merged[chunk(sub)], w_buf[2 * step + way])

    def opening(sub, carry):
        here = chunk(sub)
        for h in range(heads):
            q_rows = q_buf[h, here]
            gate_in = dot(q_rows, new_buf[h, 0:FW], 1, 1)
            up_in = dot(q_rows, new_buf[h, FW : 2 * FW], 1, 1)
            gated = (gate_in * sigmoid(gate_in) * up_in).astype(BF16)
            value = dot(gated, new_buf[h, 2 * FW : 3 * FW], 1, 1)
            norm = lax.rsqrt(jnp.mean(value * value, axis=1, keepdims=True) + 1e-06)
            merged[here, h * FW : (h + 1) * FW] = (
                att_buf[h, here].astype(F32) + value * norm
            ).astype(BF16)
        for way in range(2):
            ring_out[0, sub, way] = partial(0, sub, way).astype(BF16)
            hop(0, sub, way).start()
        return carry

    lax.fori_loop(0, SUBS, opening, 0)

    def store_out(sub):
        return pltpu.make_async_copy(out_buf.at[chunk(sub)], out_hbm.at[chunk(sub)], store_sem.at[sub])

    for step in range(1, RING):

        def middle(sub, carry, step=step):
            for way in range(2):
                mine = partial(step, sub, way)
                hop(step - 1, sub, way).wait_recv()
                value = (mine + ring_in[step - 1, sub, way].astype(F32)).astype(BF16)
                if step < RING - 1:
                    ring_out[step, sub, way] = value
                    hop(step, sub, way).start()
                else:
                    out_buf[chunk(sub), way * HALF : (way + 1) * HALF] = value
            if step == RING - 1:
                store_out(sub).start()
            return carry

        lax.fori_loop(0, SUBS, middle, 0)

    for copy in sent:
        copy.wait_send()
    for step in range(RING - 1):

        def drain(sub, carry, step=step):
            for way in range(2):
                hop(step, sub, way).wait_send()
            return carry

        lax.fori_loop(0, SUBS, drain, 0)
    for sub in range(SUBS):
        store_out(sub).wait()
    store_new.wait()


def layer(query, keys, values, code_t, fast_weights, out_weight):
    rows, width = query.shape
    heads = width // FW
    pulled = 3 * FW
    part = pulled // 2 // RING
    piece = part // RING
    sub_rows = rows // SUBS
    hops = (RING - 1) * SUBS * 2
    hbm = pl.BlockSpec(memory_space=pl.ANY)
    vmem = pl.BlockSpec(memory_space=pltpu.VMEM)
    return pl.pallas_call(
        layer_kernel,
        out_shape=(
            jax.ShapeDtypeStruct((rows, 2 * HALF), BF16),
            jax.ShapeDtypeStruct((heads, pulled, FW), BF16),
        ),
        in_specs=[hbm, hbm, hbm, vmem, hbm, hbm],
        out_specs=(hbm, hbm),
        scratch_shapes=[
            pltpu.VMEM((heads, rows, FW), BF16),
            pltpu.VMEM((heads, rows + WINDOW, FW), BF16),
            pltpu.VMEM((heads, rows + WINDOW, FW), BF16),
            pltpu.VMEM((heads, 3, FW, FW), BF16),
            pltpu.VMEM((pulled, FW), BF16),
            pltpu.VMEM((rows, 2 * FW), BF16),
            pltpu.VMEM((rows, FW), BF16),
            pltpu.VMEM((rows, FW), BF16),
            pltpu.VMEM((pulled, FW), BF16),
            pltpu.VMEM((pulled, FW), BF16),
            pltpu.VMEM((pulled, FW), BF16),
            pltpu.VMEM((RING - 1, part, FW), BF16),
            pltpu.VMEM((RING - 1, part, FW), BF16),
            pltpu.VMEM((part, FW), BF16),
            pltpu.VMEM((part, FW), BF16),
            pltpu.VMEM((RING - 1, piece, FW), BF16),
            pltpu.VMEM((RING - 1, piece, FW), BF16),
            pltpu.VMEM((heads, pulled, FW), BF16),
            pltpu.VMEM((4, heads, 128), F32),
            pltpu.VMEM((7, heads, 128), F32),
            pltpu.VMEM((heads, rows, FW), BF16),
            pltpu.VMEM((2 * RING, width, HALF), BF16),
            pltpu.VMEM((rows, width), BF16),
            pltpu.VMEM((RING - 1, SUBS, 2, sub_rows, HALF), BF16),
            pltpu.VMEM((RING - 1, SUBS, 2, sub_rows, HALF), BF16),
            pltpu.VMEM((rows, 2 * HALF), BF16),
            pltpu.SemaphoreType.DMA((8,)),
            pltpu.SemaphoreType.DMA((2 * RING,)),
            pltpu.SemaphoreType.DMA((SUBS + 1,)),
            pltpu.SemaphoreType.DMA((COPIES,)),
            pltpu.SemaphoreType.DMA((COPIES,)),
            pltpu.SemaphoreType.DMA((hops,)),
            pltpu.SemaphoreType.DMA((hops,)),
        ],
        compiler_params=pltpu.CompilerParams(
            collective_id=0, has_side_effects=True, vmem_limit_bytes=60 * MIB
        ),
        name="layer",
    )(query, keys, values, code_t, fast_weights, out_weight)


def finish_kernel(out_ref, turned_ref, final_ref, new_ref):
    final_ref[...] = out_ref[...]
    for h in range(new_ref.shape[0]):
        for m in range(3):
            new_ref[h, m] = jnp.transpose(turned_ref[h, m * FW : (m + 1) * FW])


def finish(out, turned):
    rows, width = out.shape
    heads, pulled, inner = turned.shape
    steps = 4
    out_spec = pl.BlockSpec((rows // steps, width), lambda i: (i, 0))
    return pl.pallas_call(
        finish_kernel,
        grid=(steps,),
        out_shape=(
            jax.ShapeDtypeStruct(out.shape, BF16),
            jax.ShapeDtypeStruct((heads, 3, inner, FW), BF16),
        ),
        in_specs=[out_spec, pl.BlockSpec((heads, pulled, inner // steps), lambda i: (0, 0, i))],
        out_specs=(out_spec, pl.BlockSpec((heads, 3, inner // steps, FW), lambda i: (0, 0, i, 0))),
        name="finish",
    )(out, turned)


def shards(query, keys, values, lr_code, fast_weights, out_weight):
    out, turned = layer(query, keys, values, lr_code.T, fast_weights, out_weight)
    return finish(out, turned)


def solution(mesh):
    placed = (
        P("ctx", "head"),
        P("ctx", "head"),
        P("ctx", "head"),
        P("ctx", "head"),
        P("head", None, None, None),
        P("head", None),
    )
    return jax.shard_map(
        shards,
        mesh=mesh,
        in_specs=placed,
        out_specs=(P("ctx", "head"), P("head", None, None, None)),
        check_vma=False,
    )
```

```python
import math

import jax
import jax.numpy as jnp
from jax import lax
from jax.experimental import pallas as pl
from jax.experimental.pallas import tpu as pltpu
from jax.sharding import PartitionSpec as P

FW = 512
HEAD_DIM = 128
WINDOW = 256
BASE_RATE = 0.05
BLOCK = 256
F32 = jnp.float32
BF16 = jnp.bfloat16
MESH = pl.DeviceIdType.MESH
MIB = 1024 * 1024


def dot(left, right, left_dim=1, right_dim=0):
    return lax.dot_general(
        left, right, (((left_dim,), (right_dim,)), ((), ())), preferred_element_type=F32
    )


def sigmoid(x):
    return 0.5 * jnp.tanh(0.5 * x) + 0.5


RIM_K, RIM_V, CORE_G, CORE_R = 0, 1, 2, 3
X_A, X_B, X_R = 3, 6, 9
Y_A, Y_B, Y_R = 12, 15, 18
GY_A, GY_B, GX_A, GX_B = 21, 24, 27, 30
CORE_P = 34
PAIR_Q, PAIR_ATT, WZ_A, WZ_B = 35, 36, 37, 38
W1_A, W1_B, W2_A, W2_B, W_CORE = 38, 41, 44, 47, 51
NZ_A, NZ_B = 52, 53
HY_A, HY_B, HX_A, HX_B, H_CORE = 53, 56, 59, 62, 66
COPIES = 67
RING = 4
SUBS = 2
HALF = 512


def layer_kernel(
    q_hbm, k_hbm, v_hbm, code_ref, fw_hbm, w_hbm,
    out_hbm, new_hbm,
    q_buf, k_buf, v_buf, fw_buf, base_buf, d_buf, gated_buf, pushed_buf,
    grad_out, grad_in, grad_sum, in_xa, in_xb, sum_a, sum_b, in_ya, in_yb,
    new_buf, rate_out, rate_in, att_buf, w_buf, merged, ring_out, ring_in, out_buf,
    q_pair, att_pair, w_pair, new_pair, pair_out, pair_in,
    load_sem, w_sem, store_sem, send_sem, recv_sem, ring_send, ring_recv, pair_send, pair_recv,
):
    ctx = lax.axis_index("ctx")
    me = lax.axis_index("head")
    core = lax.rem(ctx, 2)
    chip = lax.div(ctx, 2)
    y = lax.rem(chip, RING)
    x = lax.div(chip, RING)
    contexts = lax.axis_size("ctx")
    groups = lax.axis_size("head")
    rows = k_hbm.shape[0]
    tokens_all = rows * contexts
    blocks = rows // BLOCK
    part = in_xa.shape[1]
    piece = in_ya.shape[1]
    half = grad_sum.shape[0] // 2
    heads = fw_buf.shape[0]

    def at(xx, yy, cc):
        return (xx * RING + yy) * 2 + cc

    partner = at(x, y, 1 - core)
    follower = lax.rem(ctx + 1, contexts)
    leader = lax.rem(ctx + contexts - 1, contexts)
    x_peer = [None] + [at(lax.rem(x + d, RING), y, core) for d in range(1, RING)]
    y_peer = [None] + [at(x, lax.rem(y + d, RING), core) for d in range(1, RING)]
    opposite = lax.rem(me + 2, groups)
    ring_peer = (lax.rem(me + 1, groups), lax.rem(me + groups - 1, groups))

    def load(src, dst, index):
        return pltpu.make_async_copy(src, dst, load_sem.at[index])

    first, second = 1 - core, core

    def lanes(head):
        return pl.ds(pl.multiple_of(head * FW, FW), FW)

    loads = {}
    for order, head in enumerate((first, second)):
        loads["w", order] = load(fw_hbm.at[head], fw_buf.at[head], 4 * order)
        loads["k", order] = load(
            k_hbm.at[:, lanes(head)], k_buf.at[head, pl.ds(WINDOW, rows)], 4 * order + 1
        )
        loads["v", order] = load(
            v_hbm.at[:, lanes(head)], v_buf.at[head, pl.ds(WINDOW, rows)], 4 * order + 2
        )
        loads["q", order] = load(q_hbm.at[:, lanes(head)], q_buf.at[head], 4 * order + 3)
    w_loads = {}
    for step in range(RING):
        for way in range(2):
            dest = lax.rem(me + groups - 1 - step, groups) if way == 0 else lax.rem(me + 1 + step, groups)
            start = pl.multiple_of(dest * (2 * HALF) + way * HALF, HALF)
            index = 2 * step + way
            w_loads[step, way] = pltpu.make_async_copy(
                w_hbm.at[:, pl.ds(start, HALF)], w_buf.at[index], w_sem.at[index]
            )
    for order in range(2):
        for name in ("w", "k", "v"):
            loads[name, order].start()
    for step in range(2):
        for way in range(2):
            w_loads[step, way].start()
    for order in range(2):
        loads["q", order].start()

    barrier = pltpu.get_barrier_semaphore()
    ctx_peers = [follower, leader] + x_peer[1:] + y_peer[1:]
    for peer in ctx_peers:
        pl.semaphore_signal(barrier, inc=1, device_id={"ctx": peer}, device_id_type=MESH)
    head_peers = ring_peer + (opposite,)
    for peer in head_peers:
        pl.semaphore_signal(barrier, inc=1, device_id={"head": peer}, device_id_type=MESH)

    def remote(src, dst, index, peer, axis="ctx"):
        return pltpu.make_async_remote_copy(
            src_ref=src, dst_ref=dst, send_sem=send_sem.at[index], recv_sem=recv_sem.at[index],
            device_id={axis: peer}, device_id_type=MESH,
        )

    sent = []

    def send(copy):
        copy.start()
        sent.append(copy)
        return copy

    def train(head):
        def tokens(t, carry):
            start = pl.multiple_of(t * BLOCK, BLOCK)
            k_rows = k_buf[head, pl.ds(start + WINDOW, BLOCK)]
            v_rows = v_buf[head, pl.ds(start + WINDOW, BLOCK)].astype(F32)
            code_row = code_ref[pl.ds(head, 1), pl.ds(start, BLOCK)].astype(F32) * 2.0 ** (-14)
            column = jnp.transpose(jnp.broadcast_to(code_row, (8, BLOCK)))[:, 0:1]
            pushed = (column * v_rows).astype(BF16)
            gate_in = dot(k_rows, fw_buf[head, 0])
            up_in = dot(k_rows, fw_buf[head, 1])
            back = dot(pushed, fw_buf[head, 2], 1, 1)
            s = sigmoid(gate_in)
            gs = gate_in * s
            here = pl.ds(start, BLOCK)
            pushed_buf[here] = pushed
            gated_buf[here] = (gs * up_in).astype(BF16)
            d_buf[here, 0:FW] = (back * up_in * (s * (1.0 + gate_in * (1.0 - s)))).astype(BF16)
            d_buf[here, FW : 2 * FW] = (back * gs).astype(BF16)
            return carry

        lax.fori_loop(0, blocks, tokens, 0)

    def pulls(head, put):
        k_own = k_buf.at[head, pl.ds(WINDOW, rows)]
        for i in range(2 * FW // BLOCK):
            cols = pl.ds(i * BLOCK, BLOCK)
            put(cols, dot(d_buf[:, cols], k_own[...], 0, 0))
        for i in range(FW // BLOCK):
            cols = pl.ds(i * BLOCK, BLOCK)
            put(pl.ds(2 * FW + i * BLOCK, BLOCK), dot(pushed_buf[:, cols], gated_buf[...], 0, 0))

    def put_out(where, value):
        grad_out[where] = value.astype(BF16)

    def put_sum(where, value):
        grad_sum[where] = (value + grad_in[where].astype(F32)).astype(BF16)

    for name in ("w", "k", "v"):
        loads[name, 0].wait()
    train(first)
    for name in ("w", "k", "v"):
        loads[name, 1].wait()
    for step in range(2, RING):
        for way in range(2):
            w_loads[step, way].start()
    pl.semaphore_wait(barrier, len(ctx_peers) + len(head_peers))
    rim = [
        send(remote(k_buf.at[:, pl.ds(rows, WINDOW)], k_buf.at[:, pl.ds(0, WINDOW)], RIM_K, follower)),
        send(remote(v_buf.at[:, pl.ds(rows, WINDOW)], v_buf.at[:, pl.ds(0, WINDOW)], RIM_V, follower)),
    ]
    shared = rows // 2
    for step in range(2):
        for way in range(2):
            w_loads[step, way].wait()
    slice_rows = w_buf.shape[1] // contexts

    def aligned(start, size):
        return pl.ds(pl.multiple_of(start, 16), size)

    w_own_a = aligned(((core * RING + x) * RING + y) * slice_rows, slice_rows)
    w_own_b = aligned(((core * RING + y) * RING + x) * slice_rows, slice_rows)
    one, two = pl.ds(0, 2), pl.ds(2, 2)
    w_z = [
        send(remote(w_buf.at[one, w_own_a], w_pair.at[one, w_own_a], WZ_A, opposite, "head")),
        send(remote(w_buf.at[two, w_own_b], w_pair.at[two, w_own_b], WZ_B, opposite, "head")),
    ]
    for order in range(2):
        loads["q", order].wait()
    pair_q = send(remote(q_buf.at[:, pl.ds(shared, shared)], q_pair, PAIR_Q, opposite, "head"))
    pulls(first, put_out)
    core_grad = send(remote(grad_out, grad_in, CORE_G, partner))
    rate = code_ref[...].astype(F32) * 2.0 ** (-14)
    rate_out[0] = jnp.broadcast_to(jnp.sum(rate, axis=1, keepdims=True), rate_out.shape[1:])
    core_rate = send(remote(rate_out.at[0], rate_in.at[0], CORE_R, partner))
    for copy in w_z:
        copy.wait_recv()
    w_1 = []
    for d in range(1, RING):
        w_1.append(send(remote(w_pair.at[one, w_own_a], w_pair.at[one, w_own_a], W1_A + d, y_peer[d])))
        w_1.append(send(remote(w_pair.at[two, w_own_b], w_pair.at[two, w_own_b], W1_B + d, x_peer[d])))
    train(second)
    core_rate.wait_recv()
    rate_out[1] = rate_out[0] + rate_in[0]
    core_grad.wait_recv()
    pulls(second, put_sum)

    def ring_to(index):
        return lax.rem(index, RING)

    out_x = []
    for d in range(1, RING):
        out_x.append(send(remote(
            grad_sum.at[aligned(ring_to(x + d) * part, part)], in_xa.at[d - 1], X_A + d, x_peer[d])))
        out_x.append(send(remote(
            grad_sum.at[aligned(half + ring_to(y + d) * part, part)], in_xb.at[d - 1], X_B + d, y_peer[d])))
        out_x.append(send(remote(rate_out.at[1], rate_in.at[d], X_R + d, x_peer[d])))

    for m in range(3):
        base_buf[m * FW : (m + 1) * FW] = jnp.transpose(fw_buf[core, m])
    for copy in rim:
        copy.wait_recv()

    row_id = lax.broadcasted_iota(jnp.int32, (BLOCK, BLOCK), 0)
    col_id = lax.broadcasted_iota(jnp.int32, (BLOCK, BLOCK), 1)
    scale = math.log2(math.e) / math.sqrt(HEAD_DIM)

    def attend(unit, carry):
        head = lax.div(lax.rem(unit, blocks), 2)
        block = lax.rem(unit, 2) + 2 * (1 - lax.div(unit, blocks))
        start = pl.multiple_of(block * BLOCK, BLOCK)
        unseen = jnp.where((ctx == 0) & (block == 0), -1e30, 0.0).astype(F32)
        causal = col_id <= row_id
        for j in range(FW // HEAD_DIM):
            cols = pl.ds(j * HEAD_DIM, HEAD_DIM)
            q_rows = q_buf[head, pl.ds(start, BLOCK), cols]
            scores = dot(q_rows, k_buf[head, pl.ds(start, 2 * BLOCK), cols], 1, 1)
            live = jnp.where(causal, scores[:, BLOCK:], scores[:, :BLOCK] + unseen)
            top = jnp.max(live, axis=1, keepdims=True)
            exps = jnp.exp2((live - top) * scale)
            old = jnp.where(causal, 0.0, exps).astype(BF16)
            new = jnp.where(causal, exps, 0.0).astype(BF16)
            ones = jnp.ones((BLOCK, HEAD_DIM), BF16)
            v_old = jnp.concatenate([v_buf[head, pl.ds(start, BLOCK), cols], ones], 1)
            v_new = jnp.concatenate([v_buf[head, pl.ds(start + BLOCK, BLOCK), cols], ones], 1)
            both = dot(old, v_old) + dot(new, v_new)
            att_buf[head, pl.ds(start, BLOCK), cols] = (
                both[:, :HEAD_DIM] / both[:, HEAD_DIM:]
            ).astype(BF16)
        return carry

    units = 2 * blocks
    lax.fori_loop(0, units // 2, attend, 0)
    pair_att = send(remote(att_buf.at[:, pl.ds(shared, shared)], att_pair, PAIR_ATT, opposite, "head"))

    for copy in out_x:
        copy.wait_recv()

    def total(own, others):
        value = own.astype(F32)
        for i in range(RING - 1):
            value = value + others[i].astype(F32)
        return value

    sum_a[...] = total(grad_sum[aligned(x * part, part)], in_xa).astype(BF16)
    sum_b[...] = total(grad_sum[aligned(half + y * part, part)], in_xb).astype(BF16)
    rate_out[2] = rate_out[1] + rate_in[1] + rate_in[2] + rate_in[3]

    out_y = []
    for d in range(1, RING):
        out_y.append(send(remote(
            sum_a.at[aligned(ring_to(y + d) * piece, piece)], in_ya.at[d - 1], Y_A + d, y_peer[d])))
        out_y.append(send(remote(
            sum_b.at[aligned(ring_to(x + d) * piece, piece)], in_yb.at[d - 1], Y_B + d, x_peer[d])))
        out_y.append(send(remote(rate_out.at[2], rate_in.at[RING - 1 + d], Y_R + d, y_peer[d])))
    lax.fori_loop(units // 2, units // 2 + 1, attend, 0)
    for copy in out_y:
        copy.wait_recv()
    rate_out[3] = rate_out[2] + rate_in[4] + rate_in[5] + rate_in[6]
    step_size = BASE_RATE / (math.sqrt(tokens_all) * (rate_out[3, pl.ds(core, 1), 0:1] / tokens_all))

    def renorm(where, pull):
        base = base_buf[where].astype(F32)
        updated = base + step_size * pull
        old_norm = jnp.sqrt(jnp.sum(base * base, axis=1, keepdims=True) + 1e-06)
        new_norm = jnp.sqrt(jnp.sum(updated * updated, axis=1, keepdims=True) + 1e-06)
        new_buf[core, where] = (updated * (old_norm / new_norm)).astype(BF16)

    own_a = aligned(x * part + y * piece, piece)
    own_b = aligned(half + y * part + x * piece, piece)
    renorm(own_a, total(sum_a[aligned(y * piece, piece)], in_ya))
    renorm(own_b, total(sum_b[aligned(x * piece, piece)], in_yb))

    back_y = []
    for d in range(1, RING):
        mine_a, mine_b = new_buf.at[core, own_a], new_buf.at[core, own_b]
        back_y.append(send(remote(mine_a, mine_a, GY_A + d, y_peer[d])))
        back_y.append(send(remote(mine_b, mine_b, GY_B + d, x_peer[d])))
    new_z = [
        send(remote(new_buf.at[core, own_a], new_pair.at[core, own_a], NZ_A, opposite, "head")),
        send(remote(new_buf.at[core, own_b], new_pair.at[core, own_b], NZ_B, opposite, "head")),
    ]
    lax.fori_loop(units // 2 + 1, units // 2 + 2, attend, 0)
    for copy in back_y:
        copy.wait_recv()

    back_x = []
    for d in range(1, RING):
        mine_a = new_buf.at[core, aligned(x * part, part)]
        mine_b = new_buf.at[core, aligned(half + y * part, part)]
        back_x.append(send(remote(mine_a, mine_a, GX_A + d, x_peer[d])))
        back_x.append(send(remote(mine_b, mine_b, GX_B + d, y_peer[d])))
    for copy in w_1:
        copy.wait_recv()
    part_rows = slice_rows * RING
    w_2 = []
    for d in range(1, RING):
        w_x = w_pair.at[one, aligned((core * RING + x) * part_rows, part_rows)]
        w_y = w_pair.at[two, aligned((core * RING + y) * part_rows, part_rows)]
        w_2.append(send(remote(w_x, w_x, W2_A + d, x_peer[d])))
        w_2.append(send(remote(w_y, w_y, W2_B + d, y_peer[d])))
    lax.fori_loop(units // 2 + 2, units, attend, 0)
    for step in range(2, RING):
        for way in range(2):
            w_loads[step, way].wait()
    for copy in back_x:
        copy.wait_recv()
    across = send(remote(new_buf.at[core], new_buf.at[core], CORE_P, partner))
    across.wait_recv()
    store_new = pltpu.make_async_copy(new_buf, new_hbm, store_sem.at[2 * SUBS])
    store_new.start()

    sub_rows = shared // SUBS

    def hop(step, sub, way):
        index = (step * SUBS + sub) * 2 + way
        return pltpu.make_async_remote_copy(
            src_ref=ring_out.at[step, sub, way], dst_ref=ring_in.at[step, sub, way],
            send_sem=ring_send.at[index], recv_sem=ring_recv.at[index],
            device_id={"head": ring_peer[way]}, device_id_type=MESH,
        )

    def pair_hop(sub, way):
        index = sub * 2 + way
        return pltpu.make_async_remote_copy(
            src_ref=pair_out.at[sub, way], dst_ref=pair_in.at[sub, way],
            send_sem=pair_send.at[index], recv_sem=pair_recv.at[index],
            device_id={"head": ring_peer[way]}, device_id_type=MESH,
        )

    def chunk(sub):
        return pl.ds(pl.multiple_of(sub * sub_rows, sub_rows), sub_rows)

    def partial(step, sub, way):
        return dot(merged[chunk(sub)], w_buf[2 * step + way])

    merged_pair = d_buf

    def partial_pair(step, sub, way, slot):
        theirs = dot(merged_pair[chunk(sub), 0 : heads * FW], w_pair[slot])
        return partial(step, SUBS + sub, way) + theirs

    def apply(q_rows, weights, attended, h):
        gate_in = dot(q_rows, weights[h, 0:FW], 1, 1)
        up_in = dot(q_rows, weights[h, FW : 2 * FW], 1, 1)
        gated = (gate_in * sigmoid(gate_in) * up_in).astype(BF16)
        value = dot(gated, weights[h, 2 * FW : 3 * FW], 1, 1)
        norm = lax.rsqrt(jnp.mean(value * value, axis=1, keepdims=True) + 1e-06)
        return (attended.astype(F32) + value * norm).astype(BF16)

    def apply_own(sub):
        here = chunk(sub)
        for h in range(heads):
            merged[here, h * FW : (h + 1) * FW] = apply(q_buf[h, here], new_buf, att_buf[h, here], h)

    def opening(sub, carry):
        apply_own(sub)
        for way in range(2):
            ring_out[0, sub, way] = partial(0, sub, way).astype(BF16)
            hop(0, sub, way).start()
        return carry

    def store_out(sub):
        return pltpu.make_async_copy(out_buf.at[chunk(sub)], out_hbm.at[chunk(sub)], store_sem.at[sub])

    def round_ring(step):
        def middle(sub, carry):
            for way in range(2):
                mine = partial(step, sub, way)
                hop(step - 1, sub, way).wait_recv()
                value = (mine + ring_in[step - 1, sub, way].astype(F32)).astype(BF16)
                if step < RING - 1:
                    ring_out[step, sub, way] = value
                    hop(step, sub, way).start()
                else:
                    out_buf[chunk(sub), way * HALF : (way + 1) * HALF] = value
            if step == RING - 1:
                store_out(sub).start()
            return carry

        lax.fori_loop(0, SUBS, middle, 0)

    lax.fori_loop(0, SUBS, opening, 0)

    for copy in new_z:
        copy.wait_recv()
    pair_y = []
    for d in range(1, RING):
        mine_a, mine_b = new_pair.at[core, own_a], new_pair.at[core, own_b]
        pair_y.append(send(remote(mine_a, mine_a, HY_A + d, y_peer[d])))
        pair_y.append(send(remote(mine_b, mine_b, HY_B + d, x_peer[d])))

    def apply_shared(sub, carry):
        apply_own(SUBS + sub)
        return carry

    lax.fori_loop(0, SUBS, apply_shared, 0)
    for copy in pair_y:
        copy.wait_recv()
    pair_x = []
    for d in range(1, RING):
        mine_a = new_pair.at[core, aligned(x * part, part)]
        mine_b = new_pair.at[core, aligned(half + y * part, part)]
        pair_x.append(send(remote(mine_a, mine_a, HX_A + d, x_peer[d])))
        pair_x.append(send(remote(mine_b, mine_b, HX_B + d, y_peer[d])))

    round_ring(1)
    for copy in w_2:
        copy.wait_recv()
    w_half = w_pair.at[:, aligned(core * RING * part_rows, RING * part_rows)]
    w_across = send(remote(w_half, w_half, W_CORE, partner))
    round_ring(2)
    for copy in pair_x:
        copy.wait_recv()
    pair_across = send(remote(new_pair.at[core], new_pair.at[core], H_CORE, partner))
    pair_q.wait_recv()
    pair_att.wait_recv()
    w_across.wait_recv()
    pair_across.wait_recv()

    def opening_pair(sub, carry):
        here = chunk(sub)
        for h in range(heads):
            merged_pair[here, h * FW : (h + 1) * FW] = apply(
                q_pair[h, here], new_pair, att_pair[h, here], h
            )
        for way in range(2):
            pair_out[sub, way] = partial_pair(2, sub, way, way).astype(BF16)
            pair_hop(sub, way).start()
        return carry

    lax.fori_loop(0, SUBS, opening_pair, 0)
    round_ring(3)

    def closing_pair(sub, carry):
        for way in range(2):
            mine = partial_pair(3, sub, way, 2 + way)
            pair_hop(sub, way).wait_recv()
            out_buf[chunk(SUBS + sub), way * HALF : (way + 1) * HALF] = (
                mine + pair_in[sub, way].astype(F32)
            ).astype(BF16)
        store_out(SUBS + sub).start()
        return carry

    lax.fori_loop(0, SUBS, closing_pair, 0)

    for copy in sent:
        copy.wait_send()

    def drain(sub, carry):
        for way in range(2):
            for step in range(RING - 1):
                hop(step, sub, way).wait_send()
            pair_hop(sub, way).wait_send()
        return carry

    lax.fori_loop(0, SUBS, drain, 0)
    for sub in range(2 * SUBS):
        store_out(sub).wait()
    store_new.wait()


def layer(query, keys, values, code_t, fast_weights, out_weight):
    rows, width = query.shape
    heads = width // FW
    pulled = 3 * FW
    part = pulled // 2 // RING
    piece = part // RING
    shared = rows // 2
    sub_rows = shared // SUBS
    hops = (RING - 1) * SUBS * 2
    hbm = pl.BlockSpec(memory_space=pl.ANY)
    vmem = pl.BlockSpec(memory_space=pltpu.VMEM)
    return pl.pallas_call(
        layer_kernel,
        out_shape=(
            jax.ShapeDtypeStruct((rows, 2 * HALF), BF16),
            jax.ShapeDtypeStruct((heads, pulled, FW), BF16),
        ),
        in_specs=[hbm, hbm, hbm, vmem, hbm, hbm],
        out_specs=(hbm, hbm),
        scratch_shapes=[
            pltpu.VMEM((heads, rows, FW), BF16),
            pltpu.VMEM((heads, rows + WINDOW, FW), BF16),
            pltpu.VMEM((heads, rows + WINDOW, FW), BF16),
            pltpu.VMEM((heads, 3, FW, FW), BF16),
            pltpu.VMEM((pulled, FW), BF16),
            pltpu.VMEM((rows, 2 * FW), BF16),
            pltpu.VMEM((rows, FW), BF16),
            pltpu.VMEM((rows, FW), BF16),
            pltpu.VMEM((pulled, FW), BF16),
            pltpu.VMEM((pulled, FW), BF16),
            pltpu.VMEM((pulled, FW), BF16),
            pltpu.VMEM((RING - 1, part, FW), BF16),
            pltpu.VMEM((RING - 1, part, FW), BF16),
            pltpu.VMEM((part, FW), BF16),
            pltpu.VMEM((part, FW), BF16),
            pltpu.VMEM((RING - 1, piece, FW), BF16),
            pltpu.VMEM((RING - 1, piece, FW), BF16),
            pltpu.VMEM((heads, pulled, FW), BF16),
            pltpu.VMEM((4, heads, 128), F32),
            pltpu.VMEM((7, heads, 128), F32),
            pltpu.VMEM((heads, rows, FW), BF16),
            pltpu.VMEM((2 * RING, width, HALF), BF16),
            pltpu.VMEM((rows, width), BF16),
            pltpu.VMEM((RING - 1, SUBS, 2, sub_rows, HALF), BF16),
            pltpu.VMEM((RING - 1, SUBS, 2, sub_rows, HALF), BF16),
            pltpu.VMEM((rows, 2 * HALF), BF16),
            pltpu.VMEM((heads, shared, FW), BF16),
            pltpu.VMEM((heads, shared, FW), BF16),
            pltpu.VMEM((RING, width, HALF), BF16),
            pltpu.VMEM((heads, pulled, FW), BF16),
            pltpu.VMEM((SUBS, 2, sub_rows, HALF), BF16),
            pltpu.VMEM((SUBS, 2, sub_rows, HALF), BF16),
            pltpu.SemaphoreType.DMA((8,)),
            pltpu.SemaphoreType.DMA((2 * RING,)),
            pltpu.SemaphoreType.DMA((2 * SUBS + 1,)),
            pltpu.SemaphoreType.DMA((COPIES,)),
            pltpu.SemaphoreType.DMA((COPIES,)),
            pltpu.SemaphoreType.DMA((hops,)),
            pltpu.SemaphoreType.DMA((hops,)),
            pltpu.SemaphoreType.DMA((2 * SUBS,)),
            pltpu.SemaphoreType.DMA((2 * SUBS,)),
        ],
        compiler_params=pltpu.CompilerParams(
            collective_id=0, has_side_effects=True, vmem_limit_bytes=63 * MIB
        ),
        name="layer",
    )(query, keys, values, code_t, fast_weights, out_weight)


def finish_kernel(out_ref, turned_ref, final_ref, new_ref):
    final_ref[...] = out_ref[...]
    for h in range(new_ref.shape[0]):
        for m in range(3):
            new_ref[h, m] = jnp.transpose(turned_ref[h, m * FW : (m + 1) * FW])


def finish(out, turned):
    rows, width = out.shape
    heads, pulled, inner = turned.shape
    steps = 4
    out_spec = pl.BlockSpec((rows // steps, width), lambda i: (i, 0))
    return pl.pallas_call(
        finish_kernel,
        grid=(steps,),
        out_shape=(
            jax.ShapeDtypeStruct(out.shape, BF16),
            jax.ShapeDtypeStruct((heads, 3, inner, FW), BF16),
        ),
        in_specs=[out_spec, pl.BlockSpec((heads, pulled, inner // steps), lambda i: (0, 0, i))],
        out_specs=(out_spec, pl.BlockSpec((heads, 3, inner // steps, FW), lambda i: (0, 0, i, 0))),
        name="finish",
    )(out, turned)


def shards(query, keys, values, lr_code, fast_weights, out_weight):
    out, turned = layer(query, keys, values, lr_code.T, fast_weights, out_weight)
    return finish(out, turned)


def solution(mesh):
    placed = (
        P("ctx", "head"),
        P("ctx", "head"),
        P("ctx", "head"),
        P("ctx", "head"),
        P("head", None, None, None),
        P("head", None),
    )
    return jax.shard_map(
        shards,
        mesh=mesh,
        in_specs=placed,
        out_specs=(P("ctx", "head"), P("head", None, None, None)),
        check_vma=False,
    )
```

```python
import math

import jax
import jax.numpy as jnp
from jax import lax
from jax.experimental import pallas as pl
from jax.experimental.pallas import tpu as pltpu
from jax.sharding import PartitionSpec as P

FW = 512
HEAD_DIM = 128
WINDOW = 256
BASE_RATE = 0.05
BLOCK = 256
F32 = jnp.float32
BF16 = jnp.bfloat16
MESH = pl.DeviceIdType.MESH
MIB = 1024 * 1024


def dot(left, right, left_dim=1, right_dim=0):
    return lax.dot_general(
        left, right, (((left_dim,), (right_dim,)), ((), ())), preferred_element_type=F32
    )


def sigmoid(x):
    return 0.5 * jnp.tanh(0.5 * x) + 0.5


RING = 4
SHARED = 384
SUBS, SUB_ROWS = 4, 160
PAIR_SUBS, PAIR_ROWS = 2, 192
HALF = 512
COPIES = 96


def layer_kernel(
    q_hbm, k_hbm, v_hbm, code_ref, fw_hbm, w_hbm,
    out_hbm, new_hbm,
    q_buf, k_buf, v_buf, fw_buf, base_buf, d_buf, gated_buf, pushed_buf,
    grads, grad_in, in_u, sum_u, in_v,
    new_buf, rate_out, rate_in, att_buf, w_buf, merged, ring_out, ring_in, out_buf,
    q_pair, att_pair, w_pair, new_pair, pair_out, pair_in,
    load_sem, w_sem, store_sem, send_sem, recv_sem, ring_send, ring_recv, pair_send, pair_recv,
):
    ctx = lax.axis_index("ctx")
    me = lax.axis_index("head")
    core = lax.rem(ctx, 2)
    chip = lax.div(ctx, 2)
    y = lax.rem(chip, RING)
    x = lax.div(chip, RING)
    contexts = lax.axis_size("ctx")
    groups = lax.axis_size("head")
    rows = k_hbm.shape[0]
    tokens_all = rows * contexts
    blocks = rows // BLOCK
    part = in_u.shape[2]
    piece = in_v.shape[2]
    half = grads.shape[2]
    heads = fw_buf.shape[0]
    alone = rows - SHARED

    def at(xx, yy, cc):
        return (xx * RING + yy) * 2 + cc

    def ring_to(index):
        return lax.rem(index, RING)

    u = x + core * (y - x)
    v = y + core * (x - y)

    def at_uv(uu, vv):
        return at(uu + core * (vv - uu), vv + core * (uu - vv), core)

    partner = at(x, y, 1 - core)
    follower = lax.rem(ctx + 1, contexts)
    leader = lax.rem(ctx + contexts - 1, contexts)
    distances = range(1, RING)
    x_peer = [None] + [at(ring_to(x + d), y, core) for d in distances]
    y_peer = [None] + [at(x, ring_to(y + d), core) for d in distances]
    u_peer = [None] + [at_uv(ring_to(u + d), v) for d in distances]
    v_peer = [None] + [at_uv(u, ring_to(v + d)) for d in distances]
    opposite = lax.rem(me + 2, groups)
    ring_peer = (lax.rem(me + 1, groups), lax.rem(me + groups - 1, groups))

    def load(src, dst, index):
        return pltpu.make_async_copy(src, dst, load_sem.at[index])

    loads = {}
    for h in range(heads):
        lanes = pl.ds(h * FW, FW)
        loads["w", h] = load(fw_hbm.at[h], fw_buf.at[h], 4 * h)
        loads["k", h] = load(k_hbm.at[:, lanes], k_buf.at[h, pl.ds(WINDOW, rows)], 4 * h + 1)
        loads["v", h] = load(v_hbm.at[:, lanes], v_buf.at[h, pl.ds(WINDOW, rows)], 4 * h + 2)
        loads["q", h] = load(q_hbm.at[:, lanes], q_buf.at[h], 4 * h + 3)

    def w_columns(step, way):
        dest = lax.rem(me + groups - 1 - step, groups) if way == 0 else lax.rem(me + 1 + step, groups)
        return pl.ds(pl.multiple_of(dest * (2 * HALF) + way * HALF, HALF), HALF)

    w_loads = {}
    for step in range(RING):
        for way in range(2):
            index = 2 * step + way
            w_loads[step, way] = pltpu.make_async_copy(
                w_hbm.at[:, w_columns(step, way)], w_buf.at[index], w_sem.at[index]
            )
    for h in range(heads):
        for name in ("k", "v", "w"):
            loads[name, h].start()
    for h in range(heads):
        loads["q", h].start()

    barrier = pltpu.get_barrier_semaphore()
    ctx_peers = [follower, leader] + x_peer[1:] + y_peer[1:]
    for peer in ctx_peers:
        pl.semaphore_signal(barrier, inc=1, device_id={"ctx": peer}, device_id_type=MESH)
    head_peers = ring_peer + (opposite,)
    for peer in head_peers:
        pl.semaphore_signal(barrier, inc=1, device_id={"head": peer}, device_id_type=MESH)

    sent = []

    def send(src, dst, peer, axis="ctx"):
        index = len(sent)
        assert index < COPIES
        copy = pltpu.make_async_remote_copy(
            src_ref=src, dst_ref=dst, send_sem=send_sem.at[index], recv_sem=recv_sem.at[index],
            device_id={axis: peer}, device_id_type=MESH,
        )
        copy.start()
        sent.append(copy)
        return copy

    def aligned(start, size):
        return pl.ds(pl.multiple_of(start, 16), size)

    def train(head, begin, end):
        def tokens(t, carry):
            start = pl.multiple_of(t * BLOCK, BLOCK)
            k_rows = k_buf[head, pl.ds(start + WINDOW, BLOCK)]
            v_rows = v_buf[head, pl.ds(start + WINDOW, BLOCK)].astype(F32)
            code_row = code_ref[head : head + 1, pl.ds(start, BLOCK)].astype(F32) * 2.0 ** (-14)
            column = jnp.transpose(jnp.broadcast_to(code_row, (8, BLOCK)))[:, 0:1]
            pushed = (column * v_rows).astype(BF16)
            gate_in = dot(k_rows, fw_buf[head, 0])
            up_in = dot(k_rows, fw_buf[head, 1])
            back = dot(pushed, fw_buf[head, 2], 1, 1)
            s = sigmoid(gate_in)
            gs = gate_in * s
            here = pl.ds(start, BLOCK)
            pushed_buf[here] = pushed
            gated_buf[here] = (gs * up_in).astype(BF16)
            d_buf[here, 0:FW] = (back * up_in * (s * (1.0 + gate_in * (1.0 - s)))).astype(BF16)
            d_buf[here, FW : 2 * FW] = (back * gs).astype(BF16)
            return carry

        lax.fori_loop(begin, end, tokens, 0)

    def pulls(head):
        k_own = k_buf.at[head, pl.ds(WINDOW, rows)]
        per_half = half // BLOCK
        for i in range(3 * FW // BLOCK):
            if i < 2 * FW // BLOCK:
                value = dot(d_buf[:, i * BLOCK : (i + 1) * BLOCK], k_own[...], 0, 0)
            else:
                first = i * BLOCK - 2 * FW
                value = dot(pushed_buf[:, first : first + BLOCK], gated_buf[...], 0, 0)
            where = pl.ds(i % per_half * BLOCK, BLOCK)
            grads[head, i // per_half, where] = value.astype(BF16)

    def send_core(h):
        return send(grads.at[h, 1 - core], grad_in.at[h], partner)

    def send_u(h):
        grads[h, core] = (grads[h, core].astype(F32) + grad_in[h].astype(F32)).astype(BF16)
        return [
            send(grads.at[h, core, aligned(ring_to(u + d) * part, part)], in_u.at[h, d - 1], u_peer[d])
            for d in distances
        ]

    def total(own, others):
        value = own.astype(F32)
        for i in range(RING - 1):
            value = value + others[i].astype(F32)
        return value

    def send_v(h):
        sum_u[h] = total(grads[h, core, aligned(u * part, part)], in_u.at[h]).astype(BF16)
        return [
            send(sum_u.at[h, aligned(ring_to(v + d) * piece, piece)], in_v.at[h, d - 1], v_peer[d])
            for d in distances
        ]

    mine = aligned(core * half + u * part + v * piece, piece)

    def renorm(h):
        base = base_buf[h, aligned(u * part + v * piece, piece)].astype(F32)
        pull = total(sum_u[h, aligned(v * piece, piece)], in_v.at[h])
        step_size = BASE_RATE / (math.sqrt(tokens_all) * (rate_out[3, h : h + 1, 0:1] / tokens_all))
        updated = base + step_size * pull
        old_norm = jnp.sqrt(jnp.sum(base * base, axis=1, keepdims=True) + 1e-06)
        new_norm = jnp.sqrt(jnp.sum(updated * updated, axis=1, keepdims=True) + 1e-06)
        new_buf[h, mine] = (updated * (old_norm / new_norm)).astype(BF16)

    def spread_v(buf, h):
        return [send(buf.at[h, mine], buf.at[h, mine], v_peer[d]) for d in distances]

    def spread_u(buf, h):
        whole = buf.at[h, aligned(core * half + u * part, part)]
        return [send(whole, whole, u_peer[d]) for d in distances]

    def spread_core(buf, h):
        whole = buf.at[h, aligned(core * half, half)]
        return send(whole, whole, partner)

    def forward_own(h):
        whole = new_buf.at[h, aligned(core * half + u * part, part)]
        return [send(whole, whole, partner)]

    def forward(copies, h):
        out = []
        for d in (1, 3, 2):
            copies[d - 1].wait_recv()
            whole = new_buf.at[h, aligned(core * half + ring_to(u + RING - d) * part, part)]
            out.append(send(whole, whole, partner))
        return out

    def received(copies):
        for copy in copies:
            copy.wait_recv()

    row_id = lax.broadcasted_iota(jnp.int32, (BLOCK, BLOCK), 0)
    col_id = lax.broadcasted_iota(jnp.int32, (BLOCK, BLOCK), 1)
    scale = math.log2(math.e) / math.sqrt(HEAD_DIM)

    def attend(unit, carry):
        head = lax.rem(unit, heads)
        block = blocks - 1 - lax.div(unit, heads)
        start = pl.multiple_of(block * BLOCK, BLOCK)
        unseen = jnp.where((ctx == 0) & (block == 0), -1e30, 0.0).astype(F32)
        causal = col_id <= row_id
        for j in range(FW // HEAD_DIM):
            cols = pl.ds(j * HEAD_DIM, HEAD_DIM)
            q_rows = q_buf[head, pl.ds(start, BLOCK), cols]
            scores = dot(q_rows, k_buf[head, pl.ds(start, 2 * BLOCK), cols], 1, 1)
            live = jnp.where(causal, scores[:, BLOCK:], scores[:, :BLOCK] + unseen)
            top = jnp.max(live, axis=1, keepdims=True)
            exps = jnp.exp2((live - top) * scale)
            old = jnp.where(causal, 0.0, exps).astype(BF16)
            new = jnp.where(causal, exps, 0.0).astype(BF16)
            ones = jnp.ones((BLOCK, HEAD_DIM), BF16)
            v_old = jnp.concatenate([v_buf[head, pl.ds(start, BLOCK), cols], ones], 1)
            v_new = jnp.concatenate([v_buf[head, pl.ds(start + BLOCK, BLOCK), cols], ones], 1)
            both = dot(old, v_old) + dot(new, v_new)
            att_buf[head, pl.ds(start, BLOCK), cols] = (
                both[:, :HEAD_DIM] / both[:, HEAD_DIM:]
            ).astype(BF16)
        return carry

    def attention(begin, end):
        lax.fori_loop(begin, end, attend, 0)

    rate = code_ref[...].astype(F32) * 2.0 ** (-14)
    rate_out[0] = jnp.broadcast_to(jnp.sum(rate, axis=1, keepdims=True), rate_out.shape[1:])
    slice_rows = w_buf.shape[1] // contexts
    part_rows = slice_rows * RING
    w_own_a = aligned(((core * RING + x) * RING + y) * slice_rows, slice_rows)
    w_own_b = aligned(((core * RING + y) * RING + x) * slice_rows, slice_rows)
    one, two = pl.ds(0, 2), pl.ds(2, 2)

    pl.semaphore_wait(barrier, len(ctx_peers) + len(head_peers))
    edge, rim = pl.ds(rows - WINDOW, WINDOW), pl.ds(0, WINDOW)
    rims = []
    for h in range(heads):
        lanes = pl.ds(h * FW, FW)
        rims.append(send(k_hbm.at[edge, lanes], k_buf.at[h, rim], follower))
        rims.append(send(v_hbm.at[edge, lanes], v_buf.at[h, rim], follower))
    w_z = []
    for slot in range(RING):
        where = (w_own_a, w_own_b)[slot // 2]
        src = w_hbm.at[where, w_columns(slot // 2, slot % 2)]
        w_z.append(send(src, w_pair.at[slot, where], opposite, "head"))
    pair_q = []
    for h in range(heads):
        src = q_hbm.at[pl.ds(alone, SHARED), pl.ds(h * FW, FW)]
        pair_q.append(send(src, q_pair.at[h], opposite, "head"))
    core_rate = send(rate_out.at[0], rate_in.at[0], partner)
    for name in ("k", "v", "w"):
        loads[name, 0].wait()
    train(0, 0, blocks)
    for copy in w_loads.values():
        copy.start()
    pulls(0)
    core_0 = send_core(0)
    for name in ("k", "v", "w"):
        loads[name, 1].wait()
    train(1, 0, blocks)
    core_rate.wait_recv()
    rate_out[1] = rate_out[0] + rate_in[0]
    core_0.wait_recv()
    u_0 = send_u(0) + [send(rate_out.at[1], rate_in.at[d], x_peer[d]) for d in distances]
    pulls(1)
    core_1 = send_core(1)
    for h in range(heads):
        for i in range(half // BLOCK):
            block = core * (half // BLOCK) + i
            cols = pl.ds(pl.multiple_of(lax.rem(block, 2) * BLOCK, BLOCK), BLOCK)
            base_buf[h, i * BLOCK : (i + 1) * BLOCK] = jnp.transpose(fw_buf[h, lax.div(block, 2), :, cols])
    for h in range(heads):
        loads["q", h].wait()
    attention(0, 2)
    core_1.wait_recv()
    u_1 = send_u(1)
    attention(2, 4)
    pair_att = send(att_buf.at[:, pl.ds(alone, SHARED)], att_pair, opposite, "head")
    received(u_0)
    rate_out[2] = rate_out[1] + rate_in[1] + rate_in[2] + rate_in[3]
    v_0 = send_v(0) + [send(rate_out.at[2], rate_in.at[RING - 1 + d], y_peer[d]) for d in distances]
    attention(4, 5)
    received(u_1)
    v_1 = send_v(1)
    received(v_0)
    rate_out[3] = rate_out[2] + rate_in[4] + rate_in[5] + rate_in[6]
    renorm(0)
    back_0 = spread_v(new_buf, 0)
    new_z = [send(new_buf.at[0, mine], new_pair.at[0, mine], opposite, "head")]
    attention(5, 6)
    received(back_0)
    whole_0 = spread_u(new_buf, 0)
    across_0 = forward_own(0)
    received(v_1)
    renorm(1)
    back_1 = spread_v(new_buf, 1)
    new_z.append(send(new_buf.at[1, mine], new_pair.at[1, mine], opposite, "head"))
    received(rims)
    attention(6, 8)
    received(back_1)
    whole_1 = spread_u(new_buf, 1)
    across_1 = forward_own(1)
    for copy in w_loads.values():
        copy.wait()
    across_0 += forward(whole_0, 0)

    def hop(step, sub, way):
        index = (step * SUBS + sub) * 2 + way
        return pltpu.make_async_remote_copy(
            src_ref=ring_out.at[step, sub, way], dst_ref=ring_in.at[step, sub, way],
            send_sem=ring_send.at[index], recv_sem=ring_recv.at[index],
            device_id={"head": ring_peer[way]}, device_id_type=MESH,
        )

    def pair_hop(sub, way):
        index = sub * 2 + way
        return pltpu.make_async_remote_copy(
            src_ref=pair_out.at[sub, way], dst_ref=pair_in.at[sub, way],
            send_sem=pair_send.at[index], recv_sem=pair_recv.at[index],
            device_id={"head": ring_peer[way]}, device_id_type=MESH,
        )

    def chunk(sub):
        return aligned(sub * SUB_ROWS, SUB_ROWS)

    def pair_chunk(sub):
        return aligned(alone + sub * PAIR_ROWS, PAIR_ROWS)

    def partial(step, sub, way):
        return dot(merged[chunk(sub)], w_buf[2 * step + way])

    merged_pair = d_buf

    def partial_pair(step, sub, way, slot):
        theirs = merged_pair[aligned(sub * PAIR_ROWS, PAIR_ROWS), 0 : heads * FW]
        return dot(merged[pair_chunk(sub)], w_buf[2 * step + way]) + dot(theirs, w_pair[slot])

    def apply(q_rows, weights, attended, h):
        gate_in = dot(q_rows, weights[h, 0:FW], 1, 1)
        up_in = dot(q_rows, weights[h, FW : 2 * FW], 1, 1)
        gated = (gate_in * sigmoid(gate_in) * up_in).astype(BF16)
        value = dot(gated, weights[h, 2 * FW : 3 * FW], 1, 1)
        norm = lax.rsqrt(jnp.mean(value * value, axis=1, keepdims=True) + 1e-06)
        return (attended.astype(F32) + value * norm).astype(BF16)

    def apply_own(here, h):
        merged[here, h * FW : (h + 1) * FW] = apply(q_buf[h, here], new_buf, att_buf[h, here], h)

    double = 2 * SUB_ROWS

    def opening_0(pair, carry):
        apply_own(aligned(pair * double, double), 0)
        return carry

    def opening_1(pair, carry):
        apply_own(aligned(pair * double, double), 1)
        for i in range(2):
            sub = 2 * pair + i
            for way in range(2):
                ring_out[0, sub, way] = partial(0, sub, way).astype(BF16)
                hop(0, sub, way).start()
        return carry

    def store_out(here, index):
        return pltpu.make_async_copy(out_buf.at[here], out_hbm.at[here], store_sem.at[index])

    def round_ring(step, begin=0, end=SUBS):
        def middle(sub, carry):
            for way in range(2):
                own = partial(step, sub, way)
                hop(step - 1, sub, way).wait_recv()
                value = (own + ring_in[step - 1, sub, way].astype(F32)).astype(BF16)
                if step < RING - 1:
                    ring_out[step, sub, way] = value
                    hop(step, sub, way).start()
                else:
                    out_buf[chunk(sub), way * HALF : (way + 1) * HALF] = value
            if step == RING - 1:
                store_out(chunk(sub), sub).start()
            return carry

        lax.fori_loop(begin, end, middle, 0)

    received(across_0)
    lax.fori_loop(0, SUBS // 2, opening_0, 0)
    across_1 += forward(whole_1, 1)
    received(w_z)
    w_1 = []
    for d in distances:
        w_1.append(send(w_pair.at[one, w_own_a], w_pair.at[one, w_own_a], y_peer[d]))
        w_1.append(send(w_pair.at[two, w_own_b], w_pair.at[two, w_own_b], x_peer[d]))
    received(across_1)
    lax.fori_loop(0, SUBS // 2, opening_1, 0)

    received(new_z)
    pair_v = spread_v(new_pair, 0) + spread_v(new_pair, 1)
    for h in range(heads):
        apply_own(pl.ds(alone, SHARED), h)
    received(w_1)
    w_2 = []
    for d in distances:
        w_x = w_pair.at[one, aligned((core * RING + x) * part_rows, part_rows)]
        w_y = w_pair.at[two, aligned((core * RING + y) * part_rows, part_rows)]
        w_2.append(send(w_x, w_x, x_peer[d]))
        w_2.append(send(w_y, w_y, y_peer[d]))
    for h in range(heads):
        for m in range(3):
            fw_buf[h, m] = jnp.transpose(new_buf[h, m * FW : (m + 1) * FW])
    store_new = pltpu.make_async_copy(fw_buf, new_hbm, store_sem.at[SUBS + PAIR_SUBS])
    store_new.start()
    round_ring(1)
    received(pair_v)
    pair_u = spread_u(new_pair, 0) + spread_u(new_pair, 1)
    round_ring(2, 0, SUBS // 2)
    received(w_2)
    w_half = w_pair.at[:, aligned(core * RING * part_rows, RING * part_rows)]
    w_across = send(w_half, w_half, partner)
    round_ring(2, SUBS // 2, SUBS)
    received(pair_u)
    pair_across = [spread_core(new_pair, 0), spread_core(new_pair, 1)]
    received(pair_q)
    pair_att.wait_recv()
    received(pair_across)
    w_across.wait_recv()

    for h in range(heads):
        merged_pair[0:SHARED, h * FW : (h + 1) * FW] = apply(q_pair[h], new_pair, att_pair[h], h)

    def opening_pair(sub, carry):
        for way in range(2):
            pair_out[sub, way] = partial_pair(2, sub, way, way).astype(BF16)
            pair_hop(sub, way).start()
        return carry

    lax.fori_loop(0, PAIR_SUBS, opening_pair, 0)
    round_ring(3)

    def closing_pair(sub, carry):
        here = pair_chunk(sub)
        for way in range(2):
            own = partial_pair(3, sub, way, 2 + way)
            pair_hop(sub, way).wait_recv()
            out_buf[here, way * HALF : (way + 1) * HALF] = (
                own + pair_in[sub, way].astype(F32)
            ).astype(BF16)
        store_out(here, SUBS + sub).start()
        return carry

    lax.fori_loop(0, PAIR_SUBS, closing_pair, 0)

    for copy in sent:
        copy.wait_send()

    def drain(sub, carry):
        for way in range(2):
            for step in range(RING - 1):
                hop(step, sub, way).wait_send()
        return carry

    lax.fori_loop(0, SUBS, drain, 0)
    for sub in range(PAIR_SUBS):
        for way in range(2):
            pair_hop(sub, way).wait_send()
    for sub in range(SUBS):
        store_out(chunk(sub), sub).wait()
    for sub in range(PAIR_SUBS):
        store_out(pair_chunk(sub), SUBS + sub).wait()
    store_new.wait()


def layer(query, keys, values, code_t, fast_weights, out_weight):
    rows, width = query.shape
    heads = width // FW
    pulled = 3 * FW
    half = pulled // 2
    part = half // RING
    piece = part // RING
    hops = (RING - 1) * SUBS * 2
    hbm = pl.BlockSpec(memory_space=pl.ANY)
    vmem = pl.BlockSpec(memory_space=pltpu.VMEM)
    return pl.pallas_call(
        layer_kernel,
        out_shape=(
            jax.ShapeDtypeStruct((rows, 2 * HALF), BF16),
            jax.ShapeDtypeStruct(fast_weights.shape, BF16),
        ),
        in_specs=[hbm, hbm, hbm, vmem, hbm, hbm],
        out_specs=(hbm, hbm),
        scratch_shapes=[
            pltpu.VMEM((heads, rows, FW), BF16),
            pltpu.VMEM((heads, rows + WINDOW, FW), BF16),
            pltpu.VMEM((heads, rows + WINDOW, FW), BF16),
            pltpu.VMEM((heads, 3, FW, FW), BF16),
            pltpu.VMEM((heads, half, FW), BF16),
            pltpu.VMEM((rows, 2 * FW), BF16),
            pltpu.VMEM((rows, FW), BF16),
            pltpu.VMEM((rows, FW), BF16),
            pltpu.VMEM((heads, 2, half, FW), BF16),
            pltpu.VMEM((heads, half, FW), BF16),
            pltpu.VMEM((heads, RING - 1, part, FW), BF16),
            pltpu.VMEM((heads, part, FW), BF16),
            pltpu.VMEM((heads, RING - 1, piece, FW), BF16),
            pltpu.VMEM((heads, pulled, FW), BF16),
            pltpu.VMEM((4, heads, 128), F32),
            pltpu.VMEM((7, heads, 128), F32),
            pltpu.VMEM((heads, rows, FW), BF16),
            pltpu.VMEM((2 * RING, width, HALF), BF16),
            pltpu.VMEM((rows, width), BF16),
            pltpu.VMEM((RING - 1, SUBS, 2, SUB_ROWS, HALF), BF16),
            pltpu.VMEM((RING - 1, SUBS, 2, SUB_ROWS, HALF), BF16),
            pltpu.VMEM((rows, 2 * HALF), BF16),
            pltpu.VMEM((heads, SHARED, FW), BF16),
            pltpu.VMEM((heads, SHARED, FW), BF16),
            pltpu.VMEM((RING, width, HALF), BF16),
            pltpu.VMEM((heads, pulled, FW), BF16),
            pltpu.VMEM((PAIR_SUBS, 2, PAIR_ROWS, HALF), BF16),
            pltpu.VMEM((PAIR_SUBS, 2, PAIR_ROWS, HALF), BF16),
            pltpu.SemaphoreType.DMA((8,)),
            pltpu.SemaphoreType.DMA((2 * RING,)),
            pltpu.SemaphoreType.DMA((SUBS + PAIR_SUBS + 1,)),
            pltpu.SemaphoreType.DMA((COPIES,)),
            pltpu.SemaphoreType.DMA((COPIES,)),
            pltpu.SemaphoreType.DMA((hops,)),
            pltpu.SemaphoreType.DMA((hops,)),
            pltpu.SemaphoreType.DMA((2 * PAIR_SUBS,)),
            pltpu.SemaphoreType.DMA((2 * PAIR_SUBS,)),
        ],
        compiler_params=pltpu.CompilerParams(
            collective_id=0, has_side_effects=True, vmem_limit_bytes=63 * MIB
        ),
        name="layer",
    )(query, keys, values, code_t, fast_weights, out_weight)


FINISH_STEPS = 4


def finish_kernel(out_hbm, new_hbm, final_hbm, final_new_hbm, out_buf, new_buf, in_sem, out_sem):
    copies = []
    for source, target, buf in ((new_hbm, final_new_hbm, new_buf), (out_hbm, final_hbm, out_buf)):
        size = source.shape[0] // FINISH_STEPS
        for i in range(FINISH_STEPS):
            index = len(copies)
            here = pl.ds(i * size, size)
            take = pltpu.make_async_copy(source.at[here], buf.at[here], in_sem.at[index])
            take.start()
            copies.append((take, pltpu.make_async_copy(buf.at[here], target.at[here], out_sem.at[index])))
    for take, put in copies:
        take.wait()
        put.start()
    for take, put in copies:
        put.wait()


def finish(out, new_weights):
    heads, mats, inner, width = new_weights.shape
    flat = new_weights.reshape(heads * mats * inner, width)
    hbm = pl.BlockSpec(memory_space=pl.ANY)
    out, flat = pl.pallas_call(
        finish_kernel,
        out_shape=(jax.ShapeDtypeStruct(out.shape, BF16), jax.ShapeDtypeStruct(flat.shape, BF16)),
        in_specs=[hbm, hbm],
        out_specs=(hbm, hbm),
        scratch_shapes=[
            pltpu.VMEM(out.shape, BF16),
            pltpu.VMEM(flat.shape, BF16),
            pltpu.SemaphoreType.DMA((2 * FINISH_STEPS,)),
            pltpu.SemaphoreType.DMA((2 * FINISH_STEPS,)),
        ],
        name="finish",
    )(out, flat)
    return out, flat.reshape(new_weights.shape)


def shards(query, keys, values, lr_code, fast_weights, out_weight):
    out, new_weights = layer(query, keys, values, lr_code.T, fast_weights, out_weight)
    return finish(out, new_weights)


def solution(mesh):
    placed = (
        P("ctx", "head"),
        P("ctx", "head"),
        P("ctx", "head"),
        P("ctx", "head"),
        P("head", None, None, None),
        P("head", None),
    )
    return jax.shard_map(
        shards,
        mesh=mesh,
        in_specs=placed,
        out_specs=(P("ctx", "head"), P("head", None, None, None)),
        check_vma=False,
    )
```

```python
import math

import jax
import jax.numpy as jnp
from jax import lax
from jax.experimental import pallas as pl
from jax.experimental.pallas import tpu as pltpu
from jax.sharding import PartitionSpec as P

FW = 512
HEAD_DIM = 128
WINDOW = 256
BASE_RATE = 0.05
BLOCK = 256
F32 = jnp.float32
BF16 = jnp.bfloat16
MESH = pl.DeviceIdType.MESH
MIB = 1024 * 1024


def dot(left, right, left_dim=1, right_dim=0):
    return lax.dot_general(
        left, right, (((left_dim,), (right_dim,)), ((), ())), preferred_element_type=F32
    )


def sigmoid(x):
    return 0.5 * jnp.tanh(0.5 * x) + 0.5


RING = 4
SHARED = 448
SUBS, SUB_ROWS = 4, 144
PAIR_SUBS, PAIR_ROWS = 2, 224
HALF = 512
COPIES = 96


def layer_kernel(
    q_hbm, k_hbm, v_hbm, code_ref, fw_hbm, w_hbm,
    out_hbm, new_hbm,
    q_buf, k_buf, v_buf, fw_buf, base_buf, d_buf, gated_buf, pushed_buf,
    grads, grad_in, in_u, sum_u, in_v,
    new_buf, rate_out, rate_in, att_buf, w_buf, merged, ring_out, ring_in, out_buf,
    q_pair, att_pair, w_pair, new_pair, pair_out, pair_in,
    load_sem, w_sem, store_sem, send_sem, recv_sem, ring_send, ring_recv, pair_send, pair_recv,
):
    ctx = lax.axis_index("ctx")
    me = lax.axis_index("head")
    core = lax.rem(ctx, 2)
    chip = lax.div(ctx, 2)
    y = lax.rem(chip, RING)
    x = lax.div(chip, RING)
    contexts = lax.axis_size("ctx")
    groups = lax.axis_size("head")
    rows = k_hbm.shape[0]
    tokens_all = rows * contexts
    blocks = rows // BLOCK
    part = in_u.shape[2]
    piece = in_v.shape[2]
    half = grads.shape[2]
    heads = fw_buf.shape[0]
    alone = rows - SHARED

    def at(xx, yy, cc):
        return (xx * RING + yy) * 2 + cc

    def ring_to(index):
        return lax.rem(index, RING)

    u = x + core * (y - x)
    v = y + core * (x - y)

    def at_uv(uu, vv):
        return at(uu + core * (vv - uu), vv + core * (uu - vv), core)

    partner = at(x, y, 1 - core)
    follower = lax.rem(ctx + 1, contexts)
    leader = lax.rem(ctx + contexts - 1, contexts)
    distances = range(1, RING)
    x_peer = [None] + [at(ring_to(x + d), y, core) for d in distances]
    y_peer = [None] + [at(x, ring_to(y + d), core) for d in distances]
    u_peer = [None] + [at_uv(ring_to(u + d), v) for d in distances]
    v_peer = [None] + [at_uv(u, ring_to(v + d)) for d in distances]
    opposite = lax.rem(me + 2, groups)
    ring_peer = (lax.rem(me + 1, groups), lax.rem(me + groups - 1, groups))

    def load(src, dst, index):
        return pltpu.make_async_copy(src, dst, load_sem.at[index])

    loads = {}
    for h in range(heads):
        lanes = pl.ds(h * FW, FW)
        loads["w", h] = load(fw_hbm.at[h], fw_buf.at[h], 4 * h)
        loads["k", h] = load(k_hbm.at[:, lanes], k_buf.at[h, pl.ds(WINDOW, rows)], 4 * h + 1)
        loads["v", h] = load(v_hbm.at[:, lanes], v_buf.at[h, pl.ds(WINDOW, rows)], 4 * h + 2)
        loads["q", h] = load(q_hbm.at[:, lanes], q_buf.at[h], 4 * h + 3)

    def w_columns(step, way):
        dest = lax.rem(me + groups - 1 - step, groups) if way == 0 else lax.rem(me + 1 + step, groups)
        return pl.ds(pl.multiple_of(dest * (2 * HALF) + way * HALF, HALF), HALF)

    w_loads = {}
    for step in range(RING):
        for way in range(2):
            index = 2 * step + way
            w_loads[step, way] = pltpu.make_async_copy(
                w_hbm.at[:, w_columns(step, way)], w_buf.at[index], w_sem.at[index]
            )
    for h in range(heads):
        for name in ("k", "v", "w"):
            loads[name, h].start()
    for h in range(heads):
        loads["q", h].start()

    barrier = pltpu.get_barrier_semaphore()
    ctx_peers = [follower, leader] + x_peer[1:] + y_peer[1:]
    for peer in ctx_peers:
        pl.semaphore_signal(barrier, inc=1, device_id={"ctx": peer}, device_id_type=MESH)
    head_peers = ring_peer + (opposite,)
    for peer in head_peers:
        pl.semaphore_signal(barrier, inc=1, device_id={"head": peer}, device_id_type=MESH)

    sent = []

    def send(src, dst, peer, axis="ctx"):
        index = len(sent)
        assert index < COPIES
        copy = pltpu.make_async_remote_copy(
            src_ref=src, dst_ref=dst, send_sem=send_sem.at[index], recv_sem=recv_sem.at[index],
            device_id={axis: peer}, device_id_type=MESH,
        )
        copy.start()
        sent.append(copy)
        return copy

    def aligned(start, size):
        return pl.ds(pl.multiple_of(start, 16), size)

    def train(head, begin, end):
        def tokens(t, carry):
            start = pl.multiple_of(t * BLOCK, BLOCK)
            k_rows = k_buf[head, pl.ds(start + WINDOW, BLOCK)]
            v_rows = v_buf[head, pl.ds(start + WINDOW, BLOCK)].astype(F32)
            code_row = code_ref[head : head + 1, pl.ds(start, BLOCK)].astype(F32) * 2.0 ** (-14)
            column = jnp.transpose(jnp.broadcast_to(code_row, (8, BLOCK)))[:, 0:1]
            pushed = (column * v_rows).astype(BF16)
            gate_in = dot(k_rows, fw_buf[head, 0])
            up_in = dot(k_rows, fw_buf[head, 1])
            back = dot(pushed, fw_buf[head, 2], 1, 1)
            s = sigmoid(gate_in)
            gs = gate_in * s
            here = pl.ds(start, BLOCK)
            pushed_buf[here] = pushed
            gated_buf[here] = (gs * up_in).astype(BF16)
            d_buf[here, 0:FW] = (back * up_in * (s * (1.0 + gate_in * (1.0 - s)))).astype(BF16)
            d_buf[here, FW : 2 * FW] = (back * gs).astype(BF16)
            return carry

        lax.fori_loop(begin, end, tokens, 0)

    def pulls(head):
        k_own = k_buf.at[head, pl.ds(WINDOW, rows)]
        per_half = half // BLOCK
        for i in range(3 * FW // BLOCK):
            if i < 2 * FW // BLOCK:
                value = dot(d_buf[:, i * BLOCK : (i + 1) * BLOCK], k_own[...], 0, 0)
            else:
                first = i * BLOCK - 2 * FW
                value = dot(pushed_buf[:, first : first + BLOCK], gated_buf[...], 0, 0)
            where = pl.ds(i % per_half * BLOCK, BLOCK)
            grads[head, i // per_half, where] = value.astype(BF16)

    def send_core(h):
        return send(grads.at[h, 1 - core], grad_in.at[h], partner)

    def send_u(h):
        grads[h, core] = (grads[h, core].astype(F32) + grad_in[h].astype(F32)).astype(BF16)
        return [
            send(grads.at[h, core, aligned(ring_to(u + d) * part, part)], in_u.at[h, d - 1], u_peer[d])
            for d in distances
        ]

    def total(own, others):
        value = own.astype(F32)
        for i in range(RING - 1):
            value = value + others[i].astype(F32)
        return value

    def send_v(h):
        sum_u[h] = total(grads[h, core, aligned(u * part, part)], in_u.at[h]).astype(BF16)
        return [
            send(sum_u.at[h, aligned(ring_to(v + d) * piece, piece)], in_v.at[h, d - 1], v_peer[d])
            for d in distances
        ]

    mine = aligned(core * half + u * part + v * piece, piece)

    def renorm(h):
        base = base_buf[h, aligned(u * part + v * piece, piece)].astype(F32)
        pull = total(sum_u[h, aligned(v * piece, piece)], in_v.at[h])
        step_size = BASE_RATE / (math.sqrt(tokens_all) * (rate_out[3, h : h + 1, 0:1] / tokens_all))
        updated = base + step_size * pull
        old_norm = jnp.sqrt(jnp.sum(base * base, axis=1, keepdims=True) + 1e-06)
        new_norm = jnp.sqrt(jnp.sum(updated * updated, axis=1, keepdims=True) + 1e-06)
        new_buf[h, mine] = (updated * (old_norm / new_norm)).astype(BF16)

    def spread_v(buf, h):
        return [send(buf.at[h, mine], buf.at[h, mine], v_peer[d]) for d in distances]

    def spread_u(buf, h):
        whole = buf.at[h, aligned(core * half + u * part, part)]
        return [send(whole, whole, u_peer[d]) for d in distances]

    def spread_core(buf, h):
        whole = buf.at[h, aligned(core * half, half)]
        return send(whole, whole, partner)

    def forward_own(h):
        whole = new_buf.at[h, aligned(core * half + u * part, part)]
        return [send(whole, whole, partner)]

    def forward(copies, h):
        out = []
        for d in (1, 3, 2):
            copies[d - 1].wait_recv()
            whole = new_buf.at[h, aligned(core * half + ring_to(u + RING - d) * part, part)]
            out.append(send(whole, whole, partner))
        return out

    def received(copies):
        for copy in copies:
            copy.wait_recv()

    row_id = lax.broadcasted_iota(jnp.int32, (BLOCK, BLOCK), 0)
    col_id = lax.broadcasted_iota(jnp.int32, (BLOCK, BLOCK), 1)
    scale = math.log2(math.e) / math.sqrt(HEAD_DIM)

    def attend(unit, carry):
        head = lax.rem(unit, heads)
        block = blocks - 1 - lax.div(unit, heads)
        start = pl.multiple_of(block * BLOCK, BLOCK)
        unseen = jnp.where((ctx == 0) & (block == 0), -1e30, 0.0).astype(F32)
        causal = col_id <= row_id
        for j in range(FW // HEAD_DIM):
            cols = pl.ds(j * HEAD_DIM, HEAD_DIM)
            q_rows = q_buf[head, pl.ds(start, BLOCK), cols]
            scores = dot(q_rows, k_buf[head, pl.ds(start, 2 * BLOCK), cols], 1, 1)
            live = jnp.where(causal, scores[:, BLOCK:], scores[:, :BLOCK] + unseen)
            top = jnp.max(live, axis=1, keepdims=True)
            exps = jnp.exp2((live - top) * scale)
            old = jnp.where(causal, 0.0, exps).astype(BF16)
            new = jnp.where(causal, exps, 0.0).astype(BF16)
            ones = jnp.ones((BLOCK, HEAD_DIM), BF16)
            v_old = jnp.concatenate([v_buf[head, pl.ds(start, BLOCK), cols], ones], 1)
            v_new = jnp.concatenate([v_buf[head, pl.ds(start + BLOCK, BLOCK), cols], ones], 1)
            both = dot(old, v_old) + dot(new, v_new)
            att_buf[head, pl.ds(start, BLOCK), cols] = (
                both[:, :HEAD_DIM] / both[:, HEAD_DIM:]
            ).astype(BF16)
        return carry

    def attention(begin, end):
        lax.fori_loop(begin, end, attend, 0)

    rate = code_ref[...].astype(F32) * 2.0 ** (-14)
    rate_out[0] = jnp.broadcast_to(jnp.sum(rate, axis=1, keepdims=True), rate_out.shape[1:])
    slice_rows = w_buf.shape[1] // contexts
    part_rows = slice_rows * RING
    w_own_a = aligned(((core * RING + x) * RING + y) * slice_rows, slice_rows)
    w_own_b = aligned(((core * RING + y) * RING + x) * slice_rows, slice_rows)
    one, two = pl.ds(0, 2), pl.ds(2, 2)

    pl.semaphore_wait(barrier, len(ctx_peers) + len(head_peers))
    edge, rim = pl.ds(rows - WINDOW, WINDOW), pl.ds(0, WINDOW)
    rims = []
    for h in range(heads):
        lanes = pl.ds(h * FW, FW)
        rims.append(send(k_hbm.at[edge, lanes], k_buf.at[h, rim], follower))
        if h == 0:
            rims.append(send(v_hbm.at[edge, lanes], v_buf.at[h, rim], follower))
    w_z = []
    for slot in range(RING):
        where = (w_own_a, w_own_b)[slot // 2]
        src = w_hbm.at[where, w_columns(slot // 2, slot % 2)]
        w_z.append(send(src, w_pair.at[slot, where], opposite, "head"))
    pair_q = []
    for h in range(heads):
        src = q_hbm.at[pl.ds(alone, SHARED), pl.ds(h * FW, FW)]
        pair_q.append(send(src, q_pair.at[h], opposite, "head"))
    core_rate = send(rate_out.at[0], rate_in.at[0], partner)
    for name in ("k", "v", "w"):
        loads[name, 0].wait()
    train(0, 0, blocks)
    for copy in w_loads.values():
        copy.start()
    pulls(0)
    core_0 = send_core(0)
    for name in ("k", "v", "w"):
        loads[name, 1].wait()
    train(1, 0, blocks)
    core_rate.wait_recv()
    rate_out[1] = rate_out[0] + rate_in[0]
    core_0.wait_recv()
    u_0 = send_u(0) + [send(rate_out.at[1], rate_in.at[d], x_peer[d]) for d in distances]
    pulls(1)
    core_1 = send_core(1)
    for h in range(heads):
        for i in range(half // BLOCK):
            block = core * (half // BLOCK) + i
            cols = pl.ds(pl.multiple_of(lax.rem(block, 2) * BLOCK, BLOCK), BLOCK)
            base_buf[h, i * BLOCK : (i + 1) * BLOCK] = jnp.transpose(fw_buf[h, lax.div(block, 2), :, cols])
    for h in range(heads):
        loads["q", h].wait()
    attention(0, 2)
    core_1.wait_recv()
    u_1 = send_u(1)
    attention(2, 4)
    pair_att = send(att_buf.at[:, pl.ds(alone, SHARED)], att_pair, opposite, "head")
    received(u_0)
    rate_out[2] = rate_out[1] + rate_in[1] + rate_in[2] + rate_in[3]
    v_0 = send_v(0) + [send(rate_out.at[2], rate_in.at[RING - 1 + d], y_peer[d]) for d in distances]
    attention(4, 5)
    received(u_1)
    v_1 = send_v(1)
    rims.append(send(v_buf.at[1, pl.ds(rows, WINDOW)], v_buf.at[1, rim], follower))
    received(v_0)
    rate_out[3] = rate_out[2] + rate_in[4] + rate_in[5] + rate_in[6]
    renorm(0)
    back_0 = spread_v(new_buf, 0)
    new_z = [send(new_buf.at[0, mine], new_pair.at[0, mine], opposite, "head")]
    attention(5, 6)
    received(back_0)
    whole_0 = spread_u(new_buf, 0)
    across_0 = forward_own(0)
    received(v_1)
    renorm(1)
    back_1 = spread_v(new_buf, 1)
    new_z.append(send(new_buf.at[1, mine], new_pair.at[1, mine], opposite, "head"))
    received(back_1)
    whole_1 = spread_u(new_buf, 1)
    across_1 = forward_own(1)
    received(rims)
    attention(6, 8)
    for copy in w_loads.values():
        copy.wait()
    across_0 += forward(whole_0, 0)

    def hop(step, sub, way):
        index = (step * SUBS + sub) * 2 + way
        return pltpu.make_async_remote_copy(
            src_ref=ring_out.at[step, sub, way], dst_ref=ring_in.at[step, sub, way],
            send_sem=ring_send.at[index], recv_sem=ring_recv.at[index],
            device_id={"head": ring_peer[way]}, device_id_type=MESH,
        )

    def pair_hop(sub, way):
        index = sub * 2 + way
        return pltpu.make_async_remote_copy(
            src_ref=pair_out.at[sub, way], dst_ref=pair_in.at[sub, way],
            send_sem=pair_send.at[index], recv_sem=pair_recv.at[index],
            device_id={"head": ring_peer[way]}, device_id_type=MESH,
        )

    def chunk(sub):
        return aligned(sub * SUB_ROWS, SUB_ROWS)

    def pair_chunk(sub):
        return aligned(alone + sub * PAIR_ROWS, PAIR_ROWS)

    def partial(step, sub, way):
        return dot(merged[chunk(sub)], w_buf[2 * step + way])

    merged_pair = d_buf

    def partial_pair(step, sub, way, slot):
        theirs = merged_pair[aligned(sub * PAIR_ROWS, PAIR_ROWS), 0 : heads * FW]
        return dot(merged[pair_chunk(sub)], w_buf[2 * step + way]) + dot(theirs, w_pair[slot])

    def apply(q_rows, weights, attended, h):
        gate_in = dot(q_rows, weights[h, 0:FW], 1, 1)
        up_in = dot(q_rows, weights[h, FW : 2 * FW], 1, 1)
        gated = (gate_in * sigmoid(gate_in) * up_in).astype(BF16)
        value = dot(gated, weights[h, 2 * FW : 3 * FW], 1, 1)
        norm = lax.rsqrt(jnp.mean(value * value, axis=1, keepdims=True) + 1e-06)
        return (attended.astype(F32) + value * norm).astype(BF16)

    def apply_own(here, h):
        merged[here, h * FW : (h + 1) * FW] = apply(q_buf[h, here], new_buf, att_buf[h, here], h)

    double = 2 * SUB_ROWS

    def opening_0(pair, carry):
        apply_own(aligned(pair * double, double), 0)
        return carry

    def opening_1(pair, carry):
        apply_own(aligned(pair * double, double), 1)
        for i in range(2):
            sub = 2 * pair + i
            for way in range(2):
                ring_out[0, sub, way] = partial(0, sub, way).astype(BF16)
                hop(0, sub, way).start()
        return carry

    def store_out(here, index):
        return pltpu.make_async_copy(out_buf.at[here], out_hbm.at[here], store_sem.at[index])

    def round_ring(step, begin=0, end=SUBS):
        def middle(sub, carry):
            for way in range(2):
                own = partial(step, sub, way)
                hop(step - 1, sub, way).wait_recv()
                value = (own + ring_in[step - 1, sub, way].astype(F32)).astype(BF16)
                if step < RING - 1:
                    ring_out[step, sub, way] = value
                    hop(step, sub, way).start()
                else:
                    out_buf[chunk(sub), way * HALF : (way + 1) * HALF] = value
            if step == RING - 1:
                store_out(chunk(sub), sub).start()
            return carry

        lax.fori_loop(begin, end, middle, 0)

    received(across_0)
    lax.fori_loop(0, SUBS // 2, opening_0, 0)
    across_1 += forward(whole_1, 1)
    received(w_z)
    w_1 = []
    for d in distances:
        w_1.append(send(w_pair.at[one, w_own_a], w_pair.at[one, w_own_a], y_peer[d]))
        w_1.append(send(w_pair.at[two, w_own_b], w_pair.at[two, w_own_b], x_peer[d]))
    received(across_1)
    lax.fori_loop(0, SUBS // 2, opening_1, 0)

    received(new_z)
    pair_v = spread_v(new_pair, 0) + spread_v(new_pair, 1)
    for h in range(heads):
        apply_own(pl.ds(alone, SHARED), h)
    received(w_1)
    w_2 = []
    for d in distances:
        w_x = w_pair.at[one, aligned((core * RING + x) * part_rows, part_rows)]
        w_y = w_pair.at[two, aligned((core * RING + y) * part_rows, part_rows)]
        w_2.append(send(w_x, w_x, x_peer[d]))
        w_2.append(send(w_y, w_y, y_peer[d]))
    for h in range(heads):
        for m in range(3):
            fw_buf[h, m] = jnp.transpose(new_buf[h, m * FW : (m + 1) * FW])
    store_new = pltpu.make_async_copy(fw_buf, new_hbm, store_sem.at[SUBS + PAIR_SUBS])
    store_new.start()
    round_ring(1)
    received(pair_v)
    pair_u = spread_u(new_pair, 0) + spread_u(new_pair, 1)
    round_ring(2, 0, SUBS // 2)
    received(w_2)
    w_half = w_pair.at[:, aligned(core * RING * part_rows, RING * part_rows)]
    w_across = send(w_half, w_half, partner)
    round_ring(2, SUBS // 2, SUBS)
    received(pair_u)
    pair_across = [spread_core(new_pair, 0), spread_core(new_pair, 1)]
    received(pair_q)
    pair_att.wait_recv()
    received(pair_across)
    w_across.wait_recv()

    for h in range(heads):
        merged_pair[0:SHARED, h * FW : (h + 1) * FW] = apply(q_pair[h], new_pair, att_pair[h], h)

    def opening_pair(sub, carry):
        for way in range(2):
            pair_out[sub, way] = partial_pair(2, sub, way, way).astype(BF16)
            pair_hop(sub, way).start()
        return carry

    lax.fori_loop(0, PAIR_SUBS, opening_pair, 0)
    round_ring(3)

    def closing_pair(sub, carry):
        here = pair_chunk(sub)
        for way in range(2):
            own = partial_pair(3, sub, way, 2 + way)
            pair_hop(sub, way).wait_recv()
            out_buf[here, way * HALF : (way + 1) * HALF] = (
                own + pair_in[sub, way].astype(F32)
            ).astype(BF16)
        store_out(here, SUBS + sub).start()
        return carry

    lax.fori_loop(0, PAIR_SUBS, closing_pair, 0)

    for copy in sent:
        copy.wait_send()

    def drain(sub, carry):
        for way in range(2):
            for step in range(RING - 1):
                hop(step, sub, way).wait_send()
        return carry

    lax.fori_loop(0, SUBS, drain, 0)
    for sub in range(PAIR_SUBS):
        for way in range(2):
            pair_hop(sub, way).wait_send()
    for sub in range(SUBS):
        store_out(chunk(sub), sub).wait()
    for sub in range(PAIR_SUBS):
        store_out(pair_chunk(sub), SUBS + sub).wait()
    store_new.wait()


def layer(query, keys, values, code_t, fast_weights, out_weight):
    rows, width = query.shape
    heads = width // FW
    pulled = 3 * FW
    half = pulled // 2
    part = half // RING
    piece = part // RING
    hops = (RING - 1) * SUBS * 2
    hbm = pl.BlockSpec(memory_space=pl.ANY)
    vmem = pl.BlockSpec(memory_space=pltpu.VMEM)
    return pl.pallas_call(
        layer_kernel,
        out_shape=(
            jax.ShapeDtypeStruct((rows, 2 * HALF), BF16),
            jax.ShapeDtypeStruct(fast_weights.shape, BF16),
        ),
        in_specs=[hbm, hbm, hbm, vmem, hbm, hbm],
        out_specs=(hbm, hbm),
        scratch_shapes=[
            pltpu.VMEM((heads, rows, FW), BF16),
            pltpu.VMEM((heads, rows + WINDOW, FW), BF16),
            pltpu.VMEM((heads, rows + WINDOW, FW), BF16),
            pltpu.VMEM((heads, 3, FW, FW), BF16),
            pltpu.VMEM((heads, half, FW), BF16),
            pltpu.VMEM((rows, 2 * FW), BF16),
            pltpu.VMEM((rows, FW), BF16),
            pltpu.VMEM((rows, FW), BF16),
            pltpu.VMEM((heads, 2, half, FW), BF16),
            pltpu.VMEM((heads, half, FW), BF16),
            pltpu.VMEM((heads, RING - 1, part, FW), BF16),
            pltpu.VMEM((heads, part, FW), BF16),
            pltpu.VMEM((heads, RING - 1, piece, FW), BF16),
            pltpu.VMEM((heads, pulled, FW), BF16),
            pltpu.VMEM((4, heads, 128), F32),
            pltpu.VMEM((7, heads, 128), F32),
            pltpu.VMEM((heads, rows, FW), BF16),
            pltpu.VMEM((2 * RING, width, HALF), BF16),
            pltpu.VMEM((rows, width), BF16),
            pltpu.VMEM((RING - 1, SUBS, 2, SUB_ROWS, HALF), BF16),
            pltpu.VMEM((RING - 1, SUBS, 2, SUB_ROWS, HALF), BF16),
            pltpu.VMEM((rows, 2 * HALF), BF16),
            pltpu.VMEM((heads, SHARED, FW), BF16),
            pltpu.VMEM((heads, SHARED, FW), BF16),
            pltpu.VMEM((RING, width, HALF), BF16),
            pltpu.VMEM((heads, pulled, FW), BF16),
            pltpu.VMEM((PAIR_SUBS, 2, PAIR_ROWS, HALF), BF16),
            pltpu.VMEM((PAIR_SUBS, 2, PAIR_ROWS, HALF), BF16),
            pltpu.SemaphoreType.DMA((8,)),
            pltpu.SemaphoreType.DMA((2 * RING,)),
            pltpu.SemaphoreType.DMA((SUBS + PAIR_SUBS + 1,)),
            pltpu.SemaphoreType.DMA((COPIES,)),
            pltpu.SemaphoreType.DMA((COPIES,)),
            pltpu.SemaphoreType.DMA((hops,)),
            pltpu.SemaphoreType.DMA((hops,)),
            pltpu.SemaphoreType.DMA((2 * PAIR_SUBS,)),
            pltpu.SemaphoreType.DMA((2 * PAIR_SUBS,)),
        ],
        compiler_params=pltpu.CompilerParams(
            collective_id=0, has_side_effects=True, vmem_limit_bytes=63 * MIB
        ),
        name="layer",
    )(query, keys, values, code_t, fast_weights, out_weight)


FINISH_STEPS = 4


def finish_kernel(out_hbm, new_hbm, final_hbm, final_new_hbm, out_buf, new_buf, in_sem, out_sem):
    copies = []
    for source, target, buf in ((new_hbm, final_new_hbm, new_buf), (out_hbm, final_hbm, out_buf)):
        size = source.shape[0] // FINISH_STEPS
        for i in range(FINISH_STEPS):
            index = len(copies)
            here = pl.ds(i * size, size)
            take = pltpu.make_async_copy(source.at[here], buf.at[here], in_sem.at[index])
            take.start()
            copies.append((take, pltpu.make_async_copy(buf.at[here], target.at[here], out_sem.at[index])))
    for take, put in copies:
        take.wait()
        put.start()
    for take, put in copies:
        put.wait()


def finish(out, new_weights):
    heads, mats, inner, width = new_weights.shape
    flat = new_weights.reshape(heads * mats * inner, width)
    hbm = pl.BlockSpec(memory_space=pl.ANY)
    out, flat = pl.pallas_call(
        finish_kernel,
        out_shape=(jax.ShapeDtypeStruct(out.shape, BF16), jax.ShapeDtypeStruct(flat.shape, BF16)),
        in_specs=[hbm, hbm],
        out_specs=(hbm, hbm),
        scratch_shapes=[
            pltpu.VMEM(out.shape, BF16),
            pltpu.VMEM(flat.shape, BF16),
            pltpu.SemaphoreType.DMA((2 * FINISH_STEPS,)),
            pltpu.SemaphoreType.DMA((2 * FINISH_STEPS,)),
        ],
        name="finish",
    )(out, flat)
    return out, flat.reshape(new_weights.shape)


def shards(query, keys, values, lr_code, fast_weights, out_weight):
    out, new_weights = layer(query, keys, values, lr_code.T, fast_weights, out_weight)
    return finish(out, new_weights)


def solution(mesh):
    placed = (
        P("ctx", "head"),
        P("ctx", "head"),
        P("ctx", "head"),
        P("ctx", "head"),
        P("head", None, None, None),
        P("head", None),
    )
    return jax.shard_map(
        shards,
        mesh=mesh,
        in_specs=placed,
        out_specs=(P("ctx", "head"), P("head", None, None, None)),
        check_vma=False,
    )
```

```python
import math

import jax
import jax.numpy as jnp
from jax import lax
from jax.experimental import pallas as pl
from jax.experimental.pallas import tpu as pltpu
from jax.sharding import PartitionSpec as P

FW = 512
HEAD_DIM = 128
WINDOW = 256
BASE_RATE = 0.05
BLOCK = 256
F32 = jnp.float32
BF16 = jnp.bfloat16
MESH = pl.DeviceIdType.MESH
MIB = 1024 * 1024


def dot(left, right, left_dim=1, right_dim=0):
    return lax.dot_general(
        left, right, (((left_dim,), (right_dim,)), ((), ())), preferred_element_type=F32
    )


def sigmoid(x):
    return 0.5 * jnp.tanh(0.5 * x) + 0.5


RING = 4
SHARED = 448
SUBS, SUB_ROWS = 4, 144
PAIR_SUBS, PAIR_ROWS = 2, 224
HALF = 512
COPIES = 96


def layer_kernel(
    q_hbm, k_hbm, v_hbm, code_ref, fw_hbm, w_hbm,
    out_hbm, new_hbm,
    q_buf, k_buf, v_buf, fw_buf, base_buf, d_buf, gated_buf, pushed_buf,
    grads, grad_in, in_u, sum_u, in_v,
    new_buf, rate_out, rate_in, att_buf, w_buf, merged, ring_out, ring_in, out_buf,
    q_pair, att_pair, w_pair, new_pair, pair_out, pair_in,
    load_sem, w_sem, store_sem, send_sem, recv_sem, ring_send, ring_recv, pair_send, pair_recv,
):
    ctx = lax.axis_index("ctx")
    me = lax.axis_index("head")
    core = lax.rem(ctx, 2)
    chip = lax.div(ctx, 2)
    y = lax.rem(chip, RING)
    x = lax.div(chip, RING)
    contexts = lax.axis_size("ctx")
    groups = lax.axis_size("head")
    rows = k_hbm.shape[0]
    tokens_all = rows * contexts
    blocks = rows // BLOCK
    part = in_u.shape[2]
    piece = in_v.shape[2]
    half = grads.shape[2]
    heads = fw_buf.shape[0]
    alone = rows - SHARED

    def at(xx, yy, cc):
        return (xx * RING + yy) * 2 + cc

    def ring_to(index):
        return lax.rem(index, RING)

    u = x + core * (y - x)
    v = y + core * (x - y)

    def at_uv(uu, vv):
        return at(uu + core * (vv - uu), vv + core * (uu - vv), core)

    partner = at(x, y, 1 - core)
    follower = lax.rem(ctx + 1, contexts)
    leader = lax.rem(ctx + contexts - 1, contexts)
    distances = range(1, RING)
    x_peer = [None] + [at(ring_to(x + d), y, core) for d in distances]
    y_peer = [None] + [at(x, ring_to(y + d), core) for d in distances]
    u_peer = [None] + [at_uv(ring_to(u + d), v) for d in distances]
    v_peer = [None] + [at_uv(u, ring_to(v + d)) for d in distances]
    opposite = lax.rem(me + 2, groups)
    ring_peer = (lax.rem(me + 1, groups), lax.rem(me + groups - 1, groups))

    def load(src, dst, index):
        return pltpu.make_async_copy(src, dst, load_sem.at[index])

    loads = {}
    for h in range(heads):
        lanes = pl.ds(h * FW, FW)
        loads["w", h] = load(fw_hbm.at[h], fw_buf.at[h], 4 * h)
        loads["k", h] = load(k_hbm.at[:, lanes], k_buf.at[h, pl.ds(WINDOW, rows)], 4 * h + 1)
        loads["v", h] = load(v_hbm.at[:, lanes], v_buf.at[h, pl.ds(WINDOW, rows)], 4 * h + 2)
        loads["q", h] = load(q_hbm.at[:, lanes], q_buf.at[h], 4 * h + 3)

    def w_columns(step, way):
        dest = lax.rem(me + groups - 1 - step, groups) if way == 0 else lax.rem(me + 1 + step, groups)
        return pl.ds(pl.multiple_of(dest * (2 * HALF) + way * HALF, HALF), HALF)

    w_loads = {}
    for step in range(RING):
        for way in range(2):
            index = 2 * step + way
            w_loads[step, way] = pltpu.make_async_copy(
                w_hbm.at[:, w_columns(step, way)], w_buf.at[index], w_sem.at[index]
            )
    for h in range(heads):
        for name in ("k", "v", "w"):
            loads[name, h].start()
    for h in range(heads):
        loads["q", h].start()

    barrier = pltpu.get_barrier_semaphore()
    ctx_peers = [follower, leader] + x_peer[1:] + y_peer[1:]
    for peer in ctx_peers:
        pl.semaphore_signal(barrier, inc=1, device_id={"ctx": peer}, device_id_type=MESH)
    head_peers = ring_peer + (opposite,)
    for peer in head_peers:
        pl.semaphore_signal(barrier, inc=1, device_id={"head": peer}, device_id_type=MESH)

    sent = []

    def send(src, dst, peer, axis="ctx"):
        index = len(sent)
        assert index < COPIES
        copy = pltpu.make_async_remote_copy(
            src_ref=src, dst_ref=dst, send_sem=send_sem.at[index], recv_sem=recv_sem.at[index],
            device_id={axis: peer}, device_id_type=MESH,
        )
        copy.start()
        sent.append(copy)
        return copy

    def aligned(start, size):
        return pl.ds(pl.multiple_of(start, 16), size)

    def train(head, begin, end):
        def tokens(t, carry):
            start = pl.multiple_of(t * BLOCK, BLOCK)
            k_rows = k_buf[head, pl.ds(start + WINDOW, BLOCK)]
            v_rows = v_buf[head, pl.ds(start + WINDOW, BLOCK)].astype(F32)
            code_row = code_ref[head : head + 1, pl.ds(start, BLOCK)].astype(F32) * 2.0 ** (-14)
            column = jnp.transpose(jnp.broadcast_to(code_row, (8, BLOCK)))[:, 0:1]
            pushed = (column * v_rows).astype(BF16)
            gate_in = dot(k_rows, fw_buf[head, 0])
            up_in = dot(k_rows, fw_buf[head, 1])
            back = dot(pushed, fw_buf[head, 2], 1, 1)
            s = sigmoid(gate_in)
            gs = gate_in * s
            here = pl.ds(start, BLOCK)
            pushed_buf[here] = pushed
            gated_buf[here] = (gs * up_in).astype(BF16)
            d_buf[here, 0:FW] = (back * up_in * (s * (1.0 + gate_in * (1.0 - s)))).astype(BF16)
            d_buf[here, FW : 2 * FW] = (back * gs).astype(BF16)
            return carry

        lax.fori_loop(begin, end, tokens, 0)

    def pulls(head):
        k_own = k_buf.at[head, pl.ds(WINDOW, rows)]
        per_half = half // BLOCK
        for i in range(3 * FW // BLOCK):
            if i < 2 * FW // BLOCK:
                value = dot(d_buf[:, i * BLOCK : (i + 1) * BLOCK], k_own[...], 0, 0)
            else:
                first = i * BLOCK - 2 * FW
                value = dot(pushed_buf[:, first : first + BLOCK], gated_buf[...], 0, 0)
            where = pl.ds(i % per_half * BLOCK, BLOCK)
            grads[head, i // per_half, where] = value.astype(BF16)

    def send_core(h):
        return send(grads.at[h, 1 - core], grad_in.at[h], partner)

    def send_u(h):
        grads[h, core] = (grads[h, core].astype(F32) + grad_in[h].astype(F32)).astype(BF16)
        return [
            send(grads.at[h, core, aligned(ring_to(u + d) * part, part)], in_u.at[h, d - 1], u_peer[d])
            for d in distances
        ]

    def total(own, others):
        value = own.astype(F32)
        for i in range(RING - 1):
            value = value + others[i].astype(F32)
        return value

    def send_v(h):
        sum_u[h] = total(grads[h, core, aligned(u * part, part)], in_u.at[h]).astype(BF16)
        return [
            send(sum_u.at[h, aligned(ring_to(v + d) * piece, piece)], in_v.at[h, d - 1], v_peer[d])
            for d in distances
        ]

    mine = aligned(core * half + u * part + v * piece, piece)

    def renorm(h):
        base = base_buf[h, aligned(u * part + v * piece, piece)].astype(F32)
        pull = total(sum_u[h, aligned(v * piece, piece)], in_v.at[h])
        step_size = BASE_RATE / (math.sqrt(tokens_all) * (rate_out[3, h : h + 1, 0:1] / tokens_all))
        updated = base + step_size * pull
        old_norm = jnp.sqrt(jnp.sum(base * base, axis=1, keepdims=True) + 1e-06)
        new_norm = jnp.sqrt(jnp.sum(updated * updated, axis=1, keepdims=True) + 1e-06)
        new_buf[h, mine] = (updated * (old_norm / new_norm)).astype(BF16)

    def spread_v(buf, h):
        return [send(buf.at[h, mine], buf.at[h, mine], v_peer[d]) for d in distances]

    def spread_u(buf, h):
        whole = buf.at[h, aligned(core * half + u * part, part)]
        return [send(whole, whole, u_peer[d]) for d in distances]

    def spread_core(buf, h):
        whole = buf.at[h, aligned(core * half, half)]
        return send(whole, whole, partner)

    def forward_own(h):
        whole = new_buf.at[h, aligned(core * half + u * part, part)]
        return [send(whole, whole, partner)]

    def forward(copies, h):
        out = []
        for d in (1, 3, 2):
            copies[d - 1].wait_recv()
            whole = new_buf.at[h, aligned(core * half + ring_to(u + RING - d) * part, part)]
            out.append(send(whole, whole, partner))
        return out

    def received(copies):
        for copy in copies:
            copy.wait_recv()

    row_id = lax.broadcasted_iota(jnp.int32, (BLOCK, BLOCK), 0)
    col_id = lax.broadcasted_iota(jnp.int32, (BLOCK, BLOCK), 1)
    scale = math.log2(math.e) / math.sqrt(HEAD_DIM)

    def attend(unit, carry):
        head = lax.rem(unit, heads)
        block = blocks - 1 - lax.div(unit, heads)
        start = pl.multiple_of(block * BLOCK, BLOCK)
        unseen = jnp.where((ctx == 0) & (block == 0), -1e30, 0.0).astype(F32)
        causal = col_id <= row_id
        for j in range(FW // HEAD_DIM):
            cols = pl.ds(j * HEAD_DIM, HEAD_DIM)
            q_rows = q_buf[head, pl.ds(start, BLOCK), cols]
            scores = dot(q_rows, k_buf[head, pl.ds(start, 2 * BLOCK), cols], 1, 1)
            live = jnp.where(causal, scores[:, BLOCK:], scores[:, :BLOCK] + unseen)
            top = jnp.max(live, axis=1, keepdims=True)
            exps = jnp.exp2((live - top) * scale)
            old = jnp.where(causal, 0.0, exps).astype(BF16)
            new = jnp.where(causal, exps, 0.0).astype(BF16)
            ones = jnp.ones((BLOCK, HEAD_DIM), BF16)
            v_old = jnp.concatenate([v_buf[head, pl.ds(start, BLOCK), cols], ones], 1)
            v_new = jnp.concatenate([v_buf[head, pl.ds(start + BLOCK, BLOCK), cols], ones], 1)
            both = dot(old, v_old) + dot(new, v_new)
            att_buf[head, pl.ds(start, BLOCK), cols] = (
                both[:, :HEAD_DIM] / both[:, HEAD_DIM:]
            ).astype(BF16)
        return carry

    def attention(begin, end):
        lax.fori_loop(begin, end, attend, 0)

    rate = code_ref[...].astype(F32) * 2.0 ** (-14)
    rate_out[0] = jnp.broadcast_to(jnp.sum(rate, axis=1, keepdims=True), rate_out.shape[1:])
    slice_rows = w_buf.shape[1] // contexts
    part_rows = slice_rows * RING
    w_own_a = aligned(((core * RING + x) * RING + y) * slice_rows, slice_rows)
    w_own_b = aligned(((core * RING + y) * RING + x) * slice_rows, slice_rows)
    one, two = pl.ds(0, 2), pl.ds(2, 2)

    pl.semaphore_wait(barrier, len(ctx_peers) + len(head_peers))
    edge, rim = pl.ds(rows - WINDOW, WINDOW), pl.ds(0, WINDOW)
    rims = []
    for h in range(heads):
        lanes = pl.ds(h * FW, FW)
        rims.append(send(k_hbm.at[edge, lanes], k_buf.at[h, rim], follower))
        if h == 0:
            rims.append(send(v_hbm.at[edge, lanes], v_buf.at[h, rim], follower))
    w_z = []
    for slot in range(RING):
        where = (w_own_a, w_own_b)[slot // 2]
        src = w_hbm.at[where, w_columns(slot // 2, slot % 2)]
        w_z.append(send(src, w_pair.at[slot, where], opposite, "head"))
    pair_q = []
    for h in range(heads):
        src = q_hbm.at[pl.ds(alone, SHARED), pl.ds(h * FW, FW)]
        pair_q.append(send(src, q_pair.at[h], opposite, "head"))
    core_rate = send(rate_out.at[0], rate_in.at[0], partner)
    for name in ("k", "v", "w"):
        loads[name, 0].wait()
    train(0, 0, blocks)
    for copy in w_loads.values():
        copy.start()
    pulls(0)
    core_0 = send_core(0)
    for name in ("k", "v", "w"):
        loads[name, 1].wait()
    train(1, 0, blocks)
    core_rate.wait_recv()
    rate_out[1] = rate_out[0] + rate_in[0]
    core_0.wait_recv()
    u_0 = send_u(0) + [send(rate_out.at[1], rate_in.at[d], x_peer[d]) for d in distances]
    pulls(1)
    core_1 = send_core(1)
    for h in range(heads):
        for i in range(half // BLOCK):
            block = core * (half // BLOCK) + i
            cols = pl.ds(pl.multiple_of(lax.rem(block, 2) * BLOCK, BLOCK), BLOCK)
            base_buf[h, i * BLOCK : (i + 1) * BLOCK] = jnp.transpose(fw_buf[h, lax.div(block, 2), :, cols])
    for h in range(heads):
        loads["q", h].wait()
    attention(0, 2)
    core_1.wait_recv()
    u_1 = send_u(1)
    attention(2, 4)
    pair_att = send(att_buf.at[:, pl.ds(alone, SHARED)], att_pair, opposite, "head")
    received(u_0)
    rate_out[2] = rate_out[1] + rate_in[1] + rate_in[2] + rate_in[3]
    v_0 = send_v(0) + [send(rate_out.at[2], rate_in.at[RING - 1 + d], y_peer[d]) for d in distances]
    attention(4, 5)
    received(u_1)
    v_1 = send_v(1)
    rims.append(send(v_buf.at[1, pl.ds(rows, WINDOW)], v_buf.at[1, rim], follower))
    received(v_0)
    rate_out[3] = rate_out[2] + rate_in[4] + rate_in[5] + rate_in[6]
    renorm(0)
    back_0 = spread_v(new_buf, 0)
    new_z = [send(new_buf.at[0, mine], new_pair.at[0, mine], opposite, "head")]
    attention(5, 6)
    received(v_1)
    renorm(1)
    back_1 = spread_v(new_buf, 1)
    new_z.append(send(new_buf.at[1, mine], new_pair.at[1, mine], opposite, "head"))
    received(back_0)
    whole_0 = spread_u(new_buf, 0)
    across_0 = forward_own(0)
    received(back_1)
    whole_1 = spread_u(new_buf, 1)
    across_1 = forward_own(1)
    received(rims)
    attention(6, 8)
    for copy in w_loads.values():
        copy.wait()
    across_0 += forward(whole_0, 0)

    def hop(step, sub, way):
        index = (step * SUBS + sub) * 2 + way
        return pltpu.make_async_remote_copy(
            src_ref=ring_out.at[step, sub, way], dst_ref=ring_in.at[step, sub, way],
            send_sem=ring_send.at[index], recv_sem=ring_recv.at[index],
            device_id={"head": ring_peer[way]}, device_id_type=MESH,
        )

    def pair_hop(sub, way):
        index = sub * 2 + way
        return pltpu.make_async_remote_copy(
            src_ref=pair_out.at[sub, way], dst_ref=pair_in.at[sub, way],
            send_sem=pair_send.at[index], recv_sem=pair_recv.at[index],
            device_id={"head": ring_peer[way]}, device_id_type=MESH,
        )

    def chunk(sub):
        return aligned(sub * SUB_ROWS, SUB_ROWS)

    def pair_chunk(sub):
        return aligned(alone + sub * PAIR_ROWS, PAIR_ROWS)

    def partial(step, sub, way):
        return dot(merged[chunk(sub)], w_buf[2 * step + way])

    merged_pair = d_buf

    def partial_pair(step, sub, way, slot):
        theirs = merged_pair[aligned(sub * PAIR_ROWS, PAIR_ROWS), 0 : heads * FW]
        return dot(merged[pair_chunk(sub)], w_buf[2 * step + way]) + dot(theirs, w_pair[slot])

    def apply(q_rows, weights, attended, h):
        gate_in = dot(q_rows, weights[h, 0:FW], 1, 1)
        up_in = dot(q_rows, weights[h, FW : 2 * FW], 1, 1)
        gated = (gate_in * sigmoid(gate_in) * up_in).astype(BF16)
        value = dot(gated, weights[h, 2 * FW : 3 * FW], 1, 1)
        norm = lax.rsqrt(jnp.mean(value * value, axis=1, keepdims=True) + 1e-06)
        return (attended.astype(F32) + value * norm).astype(BF16)

    def apply_own(here, h):
        merged[here, h * FW : (h + 1) * FW] = apply(q_buf[h, here], new_buf, att_buf[h, here], h)

    double = 2 * SUB_ROWS

    def opening_0(pair, carry):
        apply_own(aligned(pair * double, double), 0)
        return carry

    def opening_1(sub, carry):
        apply_own(chunk(sub), 1)
        for way in range(2):
            ring_out[0, sub, way] = partial(0, sub, way).astype(BF16)
            hop(0, sub, way).start()
        return carry

    def store_out(here, index):
        return pltpu.make_async_copy(out_buf.at[here], out_hbm.at[here], store_sem.at[index])

    def round_ring(step, begin=0, end=SUBS):
        def middle(sub, carry):
            for way in range(2):
                own = partial(step, sub, way)
                hop(step - 1, sub, way).wait_recv()
                value = (own + ring_in[step - 1, sub, way].astype(F32)).astype(BF16)
                if step < RING - 1:
                    ring_out[step, sub, way] = value
                    hop(step, sub, way).start()
                else:
                    out_buf[chunk(sub), way * HALF : (way + 1) * HALF] = value
            if step == RING - 1:
                store_out(chunk(sub), sub).start()
            return carry

        lax.fori_loop(begin, end, middle, 0)

    received(across_0)
    lax.fori_loop(0, SUBS // 2, opening_0, 0)
    across_1 += forward(whole_1, 1)
    received(w_z)
    w_1 = []
    for d in distances:
        w_1.append(send(w_pair.at[one, w_own_a], w_pair.at[one, w_own_a], y_peer[d]))
        w_1.append(send(w_pair.at[two, w_own_b], w_pair.at[two, w_own_b], x_peer[d]))
    received(across_1)
    lax.fori_loop(0, SUBS, opening_1, 0)

    received(new_z)
    pair_v = spread_v(new_pair, 0) + spread_v(new_pair, 1)
    for h in range(heads):
        apply_own(pl.ds(alone, SHARED), h)
    received(w_1)
    w_2 = []
    for d in distances:
        w_x = w_pair.at[one, aligned((core * RING + x) * part_rows, part_rows)]
        w_y = w_pair.at[two, aligned((core * RING + y) * part_rows, part_rows)]
        w_2.append(send(w_x, w_x, x_peer[d]))
        w_2.append(send(w_y, w_y, y_peer[d]))
    for h in range(heads):
        for m in range(3):
            fw_buf[h, m] = jnp.transpose(new_buf[h, m * FW : (m + 1) * FW])
    store_new = pltpu.make_async_copy(fw_buf, new_hbm, store_sem.at[SUBS + PAIR_SUBS])
    store_new.start()
    round_ring(1)
    received(pair_v)
    pair_u = spread_u(new_pair, 0) + spread_u(new_pair, 1)
    round_ring(2, 0, SUBS // 2)
    received(w_2)
    w_half = w_pair.at[:, aligned(core * RING * part_rows, RING * part_rows)]
    w_across = send(w_half, w_half, partner)
    round_ring(2, SUBS // 2, SUBS)
    received(pair_u)
    pair_across = [spread_core(new_pair, 0), spread_core(new_pair, 1)]
    received(pair_q)
    pair_att.wait_recv()
    received(pair_across)
    w_across.wait_recv()

    for h in range(heads):
        merged_pair[0:SHARED, h * FW : (h + 1) * FW] = apply(q_pair[h], new_pair, att_pair[h], h)

    def opening_pair(sub, carry):
        for way in range(2):
            pair_out[sub, way] = partial_pair(2, sub, way, way).astype(BF16)
            pair_hop(sub, way).start()
        return carry

    lax.fori_loop(0, PAIR_SUBS, opening_pair, 0)
    round_ring(3)

    def closing_pair(sub, carry):
        here = pair_chunk(sub)
        for way in range(2):
            own = partial_pair(3, sub, way, 2 + way)
            pair_hop(sub, way).wait_recv()
            out_buf[here, way * HALF : (way + 1) * HALF] = (
                own + pair_in[sub, way].astype(F32)
            ).astype(BF16)
        store_out(here, SUBS + sub).start()
        return carry

    lax.fori_loop(0, PAIR_SUBS, closing_pair, 0)

    for copy in sent:
        copy.wait_send()

    def drain(sub, carry):
        for way in range(2):
            for step in range(RING - 1):
                hop(step, sub, way).wait_send()
        return carry

    lax.fori_loop(0, SUBS, drain, 0)
    for sub in range(PAIR_SUBS):
        for way in range(2):
            pair_hop(sub, way).wait_send()
    for sub in range(SUBS):
        store_out(chunk(sub), sub).wait()
    for sub in range(PAIR_SUBS):
        store_out(pair_chunk(sub), SUBS + sub).wait()
    store_new.wait()


def layer(query, keys, values, code_t, fast_weights, out_weight):
    rows, width = query.shape
    heads = width // FW
    pulled = 3 * FW
    half = pulled // 2
    part = half // RING
    piece = part // RING
    hops = (RING - 1) * SUBS * 2
    hbm = pl.BlockSpec(memory_space=pl.ANY)
    vmem = pl.BlockSpec(memory_space=pltpu.VMEM)
    return pl.pallas_call(
        layer_kernel,
        out_shape=(
            jax.ShapeDtypeStruct((rows, 2 * HALF), BF16),
            jax.ShapeDtypeStruct(fast_weights.shape, BF16),
        ),
        in_specs=[hbm, hbm, hbm, vmem, hbm, hbm],
        out_specs=(hbm, hbm),
        scratch_shapes=[
            pltpu.VMEM((heads, rows, FW), BF16),
            pltpu.VMEM((heads, rows + WINDOW, FW), BF16),
            pltpu.VMEM((heads, rows + WINDOW, FW), BF16),
            pltpu.VMEM((heads, 3, FW, FW), BF16),
            pltpu.VMEM((heads, half, FW), BF16),
            pltpu.VMEM((rows, 2 * FW), BF16),
            pltpu.VMEM((rows, FW), BF16),
            pltpu.VMEM((rows, FW), BF16),
            pltpu.VMEM((heads, 2, half, FW), BF16),
            pltpu.VMEM((heads, half, FW), BF16),
            pltpu.VMEM((heads, RING - 1, part, FW), BF16),
            pltpu.VMEM((heads, part, FW), BF16),
            pltpu.VMEM((heads, RING - 1, piece, FW), BF16),
            pltpu.VMEM((heads, pulled, FW), BF16),
            pltpu.VMEM((4, heads, 128), F32),
            pltpu.VMEM((7, heads, 128), F32),
            pltpu.VMEM((heads, rows, FW), BF16),
            pltpu.VMEM((2 * RING, width, HALF), BF16),
            pltpu.VMEM((rows, width), BF16),
            pltpu.VMEM((RING - 1, SUBS, 2, SUB_ROWS, HALF), BF16),
            pltpu.VMEM((RING - 1, SUBS, 2, SUB_ROWS, HALF), BF16),
            pltpu.VMEM((rows, 2 * HALF), BF16),
            pltpu.VMEM((heads, SHARED, FW), BF16),
            pltpu.VMEM((heads, SHARED, FW), BF16),
            pltpu.VMEM((RING, width, HALF), BF16),
            pltpu.VMEM((heads, pulled, FW), BF16),
            pltpu.VMEM((PAIR_SUBS, 2, PAIR_ROWS, HALF), BF16),
            pltpu.VMEM((PAIR_SUBS, 2, PAIR_ROWS, HALF), BF16),
            pltpu.SemaphoreType.DMA((8,)),
            pltpu.SemaphoreType.DMA((2 * RING,)),
            pltpu.SemaphoreType.DMA((SUBS + PAIR_SUBS + 1,)),
            pltpu.SemaphoreType.DMA((COPIES,)),
            pltpu.SemaphoreType.DMA((COPIES,)),
            pltpu.SemaphoreType.DMA((hops,)),
            pltpu.SemaphoreType.DMA((hops,)),
            pltpu.SemaphoreType.DMA((2 * PAIR_SUBS,)),
            pltpu.SemaphoreType.DMA((2 * PAIR_SUBS,)),
        ],
        compiler_params=pltpu.CompilerParams(
            collective_id=0, has_side_effects=True, vmem_limit_bytes=63 * MIB
        ),
        name="layer",
    )(query, keys, values, code_t, fast_weights, out_weight)


FINISH_STEPS = 2


def finish_kernel(out_hbm, new_hbm, final_hbm, final_new_hbm, out_buf, new_buf, in_sem, out_sem):
    copies = []
    for source, target, buf in ((new_hbm, final_new_hbm, new_buf), (out_hbm, final_hbm, out_buf)):
        size = source.shape[0] // FINISH_STEPS
        for i in range(FINISH_STEPS):
            index = len(copies)
            here = pl.ds(i * size, size)
            take = pltpu.make_async_copy(source.at[here], buf.at[here], in_sem.at[index])
            take.start()
            copies.append((take, pltpu.make_async_copy(buf.at[here], target.at[here], out_sem.at[index])))
    for take, put in copies:
        take.wait()
        put.start()
    for take, put in copies:
        put.wait()


def finish(out, new_weights):
    heads, mats, inner, width = new_weights.shape
    flat = new_weights.reshape(heads * mats * inner, width)
    hbm = pl.BlockSpec(memory_space=pl.ANY)
    out, flat = pl.pallas_call(
        finish_kernel,
        out_shape=(jax.ShapeDtypeStruct(out.shape, BF16), jax.ShapeDtypeStruct(flat.shape, BF16)),
        in_specs=[hbm, hbm],
        out_specs=(hbm, hbm),
        scratch_shapes=[
            pltpu.VMEM(out.shape, BF16),
            pltpu.VMEM(flat.shape, BF16),
            pltpu.SemaphoreType.DMA((2 * FINISH_STEPS,)),
            pltpu.SemaphoreType.DMA((2 * FINISH_STEPS,)),
        ],
        name="finish",
    )(out, flat)
    return out, flat.reshape(new_weights.shape)


def shards(query, keys, values, lr_code, fast_weights, out_weight):
    out, new_weights = layer(query, keys, values, lr_code.T, fast_weights, out_weight)
    return finish(out, new_weights)


def solution(mesh):
    placed = (
        P("ctx", "head"),
        P("ctx", "head"),
        P("ctx", "head"),
        P("ctx", "head"),
        P("head", None, None, None),
        P("head", None),
    )
    return jax.shard_map(
        shards,
        mesh=mesh,
        in_specs=placed,
        out_specs=(P("ctx", "head"), P("head", None, None, None)),
        check_vma=False,
    )
```
